128 devices in a mesh: grp: 4 (over y), shard: 32 (over x, z, core).
Axes of the slice: x: 4, y: 4, z: 4, core: 2. Of those that a mesh axis runs over, the one named last changes fastest.
Arguments:
- candidates: int32 [32768, 16], P(('grp', 'shard')), may hold values from 0 to 3199
- affinity: float32 [32768, 2048], P(('grp', 'shard')), may hold values from -6 to 6
- exposure: float32 [32768, 2048], P(('grp', 'shard')), may hold values from 0.5 to 2
- lengths: int32 [32768], P(('grp', 'shard')), may hold values from 256 to 2048, as said below
- item_limit: float32 [409600], P('shard'), may hold values from 0.02 to 0.2
- item_duals: float32 [409600], P('shard'), may hold values from 0 to 1
Outputs:
- primal: float32 [32768, 2048], P(('grp', 'shard'))
- duals_out: float32 [409600], P('shard')
The draws below stay inside these ranges and needn't reach their ends.
Inputs may be any that keep to these rules, and one draw needn't show every extreme that they name: `lengths`: multiples of 128; among the members of every device at least one has 2048 live slots.
All inputs are finite; a program needn't handle non-finite values.
Results may differ from the reference program's by a relative error of at most 0.0003.
Values sent between devices are 32-bit elements; how exact they have to be, the bound alone decides.
No kernel may reach another device: no remote copies, remote signals or barrier semaphores. Data moves between devices by JAX's collectives and lax.ppermute only.
A program may use at most 64 MiB of HBM per device.

```python
import math
import jax
import jax.numpy as jnp
from jax import lax

M_DEV = 256
LMAX = 2048
BLOCK = 128
ITEMS = 409600
ITERS = 2
BISECT = 16
MEMBERS = 32768


def draw_lengths(key, part):
    blocks = jax.random.randint(jax.random.fold_in(key, 17), (MEMBERS,), 2, LMAX // BLOCK + 1)
    devices = MEMBERS // M_DEV
    full_row = jax.random.randint(jax.random.fold_in(key, 29), (devices,), 0, M_DEV)
    rows = jnp.arange(MEMBERS, dtype=jnp.int32)
    owner = rows // M_DEV
    within = rows % M_DEV
    chosen = full_row[owner]
    result = jnp.where(within == chosen, LMAX // BLOCK, blocks)
    return (result * BLOCK).astype(jnp.int32)


def draw_affinity(key, part):
    log_scale = jax.random.uniform(jax.random.fold_in(key, 41), (MEMBERS, 1), jnp.float32, -4.0, 0.6)
    noise_key = jax.random.fold_in(key, 43)
    base = jax.random.normal(noise_key, (MEMBERS, LMAX), jnp.float32)
    return jnp.clip(base * jnp.exp(log_scale), -6.0, 6.0).astype(jnp.float32)


def touch_ends(entries, key, least, largest):
    longest = entries.shape.index(max(entries.shape))
    spots = []
    for shift in (0, 1):
        where = [jax.random.randint(jax.random.fold_in(key, axis), (), 0, length) for axis, length in enumerate(entries.shape)]
        where[longest] = (where[longest] + shift) % entries.shape[longest]
        spots.append(tuple(where))
    return entries.at[spots[0]].set(least).at[spots[1]].set(largest)


def level_of(rng, extent, pieces, low, high):
    def one(axis_at, parts):
        heights = jax.random.uniform(jax.random.fold_in(jax.random.fold_in(rng, 6), axis_at), (parts,), jnp.float32, low / len(pieces), high / len(pieces))
        return jnp.repeat(jnp.exp(heights), extent[axis_at] // parts).reshape((-1,) + (1,) * (len(extent) - axis_at - 1))

    factor_of = one(*pieces[0])
    for cut in pieces[1:]:
        factor_of = factor_of * one(*cut)
    return factor_of


def setup_inputs(seed: int = 0) -> dict:
    streams_of = jax.random.split(jax.random.key(seed), 7)
    candidates = touch_ends(jax.random.randint(streams_of[0], (MEMBERS, LMAX // BLOCK), 0, ITEMS // BLOCK), jax.random.fold_in(streams_of[0], 1), 0, (ITEMS // BLOCK) - 1).astype(jnp.int32)
    affinity = draw_affinity(jax.random.fold_in(streams_of[6], 71), 0)
    exposure = jnp.clip(jnp.exp(math.log(2.0) - 1.3862944 * jax.random.uniform(streams_of[2], (MEMBERS, LMAX), jnp.float32) ** level_of(streams_of[2], (MEMBERS, LMAX), ((0, 128),), -0.2, 0.2)), 0.5, 2.0)
    lengths = draw_lengths(jax.random.fold_in(streams_of[6], 71), 0)
    item_limit = jnp.clip(jnp.exp(math.log(0.2) - 2.3025851 * jax.random.uniform(streams_of[4], (ITEMS,), jnp.float32) ** level_of(streams_of[4], (ITEMS,), ((0, 32),), -0.2, 0.2)), 0.02, 0.2)
    item_duals = jnp.clip(1.0 * jax.random.uniform(streams_of[5], (ITEMS,), jnp.float32) ** level_of(streams_of[5], (ITEMS,), ((0, 32),), -0.2, 0.2), 0.0, 1.0)
    return {"candidates": candidates, "affinity": affinity, "exposure": exposure, "lengths": lengths, "item_limit": item_limit, "item_duals": item_duals}


gamma_reg = 0.5
step_eta = 0.5

def project(scaled, live_mask):
    zero_f = jnp.zeros((), jnp.float32)
    lowest = jnp.asarray(-1e+30, jnp.float32)

    def filled(thresh):
        return lax.optimization_barrier(jnp.sum(jnp.where(live_mask, jnp.clip(scaled - thresh[:, None], 0.0, 1.0), zero_f), axis=1))
    upper_t = lax.optimization_barrier(jnp.max(jnp.where(live_mask, scaled, lowest), axis=1))
    lower_t = jnp.zeros_like(upper_t)
    for _ in range(BISECT):
        middle = (lower_t + upper_t) * 0.5
        bigger = filled(middle) > 1.0
        lower_t = jnp.where(bigger, middle, lower_t)
        upper_t = jnp.where(bigger, upper_t, middle)
    return jnp.where(live_mask, jnp.clip(scaled - upper_t[:, None], 0.0, 1.0), zero_f)

def reference(candidates, affinity, exposure, lengths, item_limit, item_duals):
    members, slots = affinity.shape
    positions = jnp.arange(slots, dtype=jnp.int32)
    live_mask = positions[None, :] < lengths[:, None]
    block_rows = item_limit.shape[0] // BLOCK
    flat_blocks = candidates.reshape(-1)
    duals = item_duals
    primal = affinity
    for _ in range(ITERS):
        slot_duals = duals.reshape(block_rows, BLOCK)[flat_blocks].reshape(members, slots)
        scaled = (affinity - exposure * slot_duals) / gamma_reg
        primal = project(scaled, live_mask)
        contrib = (exposure * primal).reshape(-1, BLOCK)
        item_load = jnp.zeros((block_rows, BLOCK), jnp.float32).at[flat_blocks].add(contrib).reshape(-1)
        gradient = item_load - item_limit
        scale = jnp.sqrt(jnp.sum(gradient * gradient) / item_limit.shape[0] + 1e-06)
        duals = jnp.maximum(duals + step_eta * gradient / scale, 0.0)
    return (primal, duals)
```

```python
import jax
import jax.numpy as jnp
from jax import lax
from jax.experimental import pallas as pl
from jax.experimental.pallas import tpu as pltpu
from jax.sharding import PartitionSpec as P

BLOCK = 128
BISECT = 16
SUB = 8
BATCH = 32
COPIES = 4
DEAD = -1e30

AXES = ("grp", "shard")


def pad8(n):
    return -(-n // SUB) * SUB


def iteration_kernel(second, groups, blocks, half, item_count):
    full = 2 * half
    members = groups * SUB
    table_vregs = full // SUB

    def body(*refs):
        if second:
            (gidx, sidx, ncopy, own_d, other_d, own_g, other_g, aff, exp, nlive,
             keep, send, primal, sumsq, table, work, scaled, acc, lo, up, fills) = refs
        else:
            (gidx, sidx, ncopy, own_d, other_d, aff, exp, nlive,
             keep, send, table, work, scaled, acc, lo, up, fills) = refs

        if second:
            def square(i, s):
                r = pl.multiple_of(i * SUB, SUB)
                a = own_g[pl.ds(r, SUB), :]
                b = other_g[pl.ds(r, SUB), :]
                return s + (a * a + b * b)

            s = lax.fori_loop(0, half // SUB, square, jnp.zeros((SUB, BLOCK), jnp.float32), unroll=8)
            total = jnp.sum(jnp.sum(s, axis=1, keepdims=True), axis=0, keepdims=True)
            sumsq[...] = jnp.broadcast_to(total, (SUB, BLOCK))
            scale = jnp.sqrt(jnp.broadcast_to(total, (SUB, BLOCK)) / item_count + 1e-6)

            def fill_table(i, c):
                r = pl.multiple_of(i * SUB, SUB)
                for d, g, off in ((own_d, own_g, 0), (other_d, other_g, half)):
                    table[pl.ds(r + off, SUB), :] = jnp.maximum(
                        d[pl.ds(r, SUB), :] + 0.5 * g[pl.ds(r, SUB), :] / scale, 0.0)
                return c
        else:
            def fill_table(i, c):
                r = pl.multiple_of(i * SUB, SUB)
                table[pl.ds(r, SUB), :] = own_d[pl.ds(r, SUB), :]
                table[pl.ds(r + half, SUB), :] = other_d[pl.ds(r, SUB), :]
                return c

        lax.fori_loop(0, half // SUB, fill_table, 0, unroll=8)

        def gather(g, c):
            base = g * (SUB * blocks)
            live = nlive[pl.ds(pl.multiple_of(g * SUB, SUB), SUB), :]
            peak = jnp.full((SUB, BLOCK), DEAD, jnp.float32)
            for b in range(blocks):
                r0 = pl.multiple_of(base + b * SUB, SUB)
                for s in range(SUB):
                    work[pl.ds(r0 + s, 1), :] = table[pl.ds(gidx[base + s * blocks + b], 1), :]
                rows = pl.ds(r0, SUB)
                v = (aff[rows, :] - exp[rows, :] * work[rows, :]) * 2.0
                v = jnp.where(live > b, v, DEAD)
                scaled[rows, :] = v
                peak = jnp.maximum(peak, v)
            rows = pl.ds(pl.multiple_of(g * SUB, SUB), SUB)
            up[rows, :] = jnp.broadcast_to(jnp.max(peak, axis=1, keepdims=True), (SUB, BLOCK))
            lo[rows, :] = jnp.zeros((SUB, BLOCK), jnp.float32)
            return c

        lax.fori_loop(0, groups, gather, 0)

        def bisect(p, c):
            for g in range(groups):
                rows = pl.ds(g * SUB, SUB)
                mid = (lo[rows, :] + up[rows, :]) * 0.5
                a = None
                for b in range(blocks):
                    v = jnp.clip(scaled[pl.ds((g * blocks + b) * SUB, SUB), :] - mid, 0.0, 1.0)
                    a = v if a is None else a + v
                fill = jnp.broadcast_to(jnp.sum(a, axis=1, keepdims=True), (SUB, BLOCK))
                bigger = fill > 1.0
                lo[rows, :] = jnp.where(bigger, mid, lo[rows, :])
                up[rows, :] = jnp.where(bigger, up[rows, :], mid)
            return c

        lax.fori_loop(0, BISECT, bisect, 0)

        def allocate(g, c):
            th = up[pl.ds(pl.multiple_of(g * SUB, SUB), SUB), :]
            live = nlive[pl.ds(pl.multiple_of(g * SUB, SUB), SUB), :]
            for b in range(blocks):
                rows = pl.ds(pl.multiple_of((g * blocks + b) * SUB, SUB), SUB)
                x = jnp.where(live > b, jnp.clip(scaled[rows, :] - th, 0.0, 1.0), 0.0)
                if second:
                    primal[rows, :] = x
                work[rows, :] = exp[rows, :] * x
            return c

        lax.fori_loop(0, groups, allocate, 0)

        zero = jnp.zeros((SUB, BLOCK), jnp.float32)
        n = ncopy[0]

        def clear(i, c):
            acc[pl.ds(pl.multiple_of(i * SUB, SUB), SUB), :] = zero
            return c

        fast = n <= COPIES
        used = jnp.where(fast, n, 1)

        def clear_copy(t, c):
            return lax.fori_loop(0, table_vregs, lambda i, c: clear(t * table_vregs + i, c), c, unroll=16)

        lax.fori_loop(0, used, clear_copy, 0)

        per_member = BATCH // blocks

        @pl.when(fast)
        def _():
            def scatter(g, c):
                for q in range(SUB // per_member):
                    where = []
                    for s in range(q * per_member, (q + 1) * per_member):
                        for b in range(blocks):
                            where.append((sidx[g * (SUB * blocks) + s * blocks + b],
                                          g * (SUB * blocks) + b * SUB + s))
                    sums = [acc[pl.ds(i, 1), :] + work[pl.ds(r, 1), :] for i, r in where]
                    for (i, _), v in zip(where, sums):
                        acc[pl.ds(i, 1), :] = v
                return c

            lax.fori_loop(0, groups, scatter, 0)

        @pl.when(jnp.logical_not(fast))
        def _():
            def one(k, c):
                m = k // blocks
                b = k - m * blocks
                g = m // SUB
                r = (g * blocks + b) * SUB + (m - g * SUB)
                i = gidx[k]
                acc[pl.ds(i, 1), :] = acc[pl.ds(i, 1), :] + work[pl.ds(r, 1), :]
                return c

            lax.fori_loop(0, members * blocks, one, 0)

        def finish(i, c):
            r = pl.multiple_of(i * SUB, SUB)

            def more(t, v):
                o = pl.multiple_of(t * full + r, SUB)
                return (v[0] + acc[pl.ds(o, SUB), :], v[1] + acc[pl.ds(o + half, SUB), :])

            v = (acc[pl.ds(r, SUB), :], acc[pl.ds(r + half, SUB), :])
            keep[pl.ds(r, SUB), :], send[pl.ds(r, SUB), :] = v
            return c

        lax.fori_loop(0, half // SUB, finish, 0, unroll=8)

        def finish_more(t, c):
            def add(i, c):
                r = pl.multiple_of(i * SUB, SUB)
                o = pl.multiple_of(t * full + r, SUB)
                keep[pl.ds(r, SUB), :] += acc[pl.ds(o, SUB), :]
                send[pl.ds(r, SUB), :] += acc[pl.ds(o + half, SUB), :]
                return c

            return lax.fori_loop(0, half // SUB, add, c, unroll=8)

        lax.fori_loop(1, used, finish_more, 0)

    rows = members * blocks
    f32 = jnp.float32
    smem = pl.BlockSpec(memory_space=pltpu.SMEM)
    vmem = pl.BlockSpec(memory_space=pltpu.VMEM)
    outs = [jax.ShapeDtypeStruct((half, BLOCK), f32)] * 2
    if second:
        outs += [jax.ShapeDtypeStruct((rows, BLOCK), f32), jax.ShapeDtypeStruct((SUB, BLOCK), f32)]
    return pl.pallas_call(
        body,
        out_shape=outs,
        in_specs=[smem] * 3 + [vmem] * (7 if second else 5),
        out_specs=[vmem] * len(outs),
        scratch_shapes=[
            pltpu.VMEM((full, BLOCK), f32),
            pltpu.VMEM((rows, BLOCK), f32),
            pltpu.VMEM((rows, BLOCK), f32),
            pltpu.VMEM((COPIES * full, BLOCK), f32),
            pltpu.VMEM((members, BLOCK), f32),
            pltpu.VMEM((members, BLOCK), f32),
            pltpu.VMEM((SUB, BLOCK), f32),
        ],
        name="iterate2" if second else "iterate1",
    )


def local(candidates, affinity, exposure, lengths, item_limit, item_duals, *, grp_size, shard_size):
    chips = shard_size // 2
    same_core = [[2 * p + c for p in range(chips)] for c in range(2)]
    swap = [(g * shard_size + s, g * shard_size + (s ^ 1)) for g in range(grp_size) for s in range(shard_size)]
    members, slots = affinity.shape
    blocks = slots // BLOCK
    groups = members // SUB
    own_items = item_limit.shape[0]
    item_count = own_items * shard_size
    own_rows = own_items // BLOCK
    padded = pad8(own_rows)
    half = chips * padded
    full = 2 * half
    core = lax.axis_index("shard") % 2

    def swap_cores(x):
        return lax.ppermute(x, AXES, swap)

    def as_rows(x):
        return x.reshape(groups, SUB, blocks, BLOCK).transpose(0, 2, 1, 3).reshape(-1, BLOCK)

    def own_block(x):
        return jnp.pad(x.reshape(own_rows, BLOCK), ((0, padded - own_rows), (0, 0)))

    def gather_halves(x):
        every = lax.all_to_all(
            jnp.broadcast_to(x[None], (chips, padded, BLOCK)), "shard", 0, 0,
            axis_index_groups=same_core, tiled=True).reshape(half, BLOCK)
        return every, swap_cores(every)

    def reduce_loads(keep, send):
        chip = keep + swap_cores(send)
        plane = lax.all_to_all(
            chip.reshape(chips, padded, BLOCK), "shard", 0, 0,
            axis_index_groups=same_core, tiled=True).sum(axis=0)
        shifted = [
            lax.ppermute(plane, "grp", [(g, (g + d) % grp_size) for g in range(grp_size)])
            for d in range(1, grp_size)
        ]
        return (plane + shifted[1]) + (shifted[0] + shifted[2])

    shard_of = candidates // own_rows
    gidx = (jnp.where(shard_of % 2 == core, 0, half) + (shard_of // 2) * padded + candidates % own_rows).reshape(-1)
    batch = gidx.reshape(-1, BATCH)
    earlier = jnp.arange(BATCH)[:, None] > jnp.arange(BATCH)[None, :]
    copy = jnp.sum((batch[:, :, None] == batch[:, None, :]) & earlier, axis=2, dtype=jnp.int32)
    sidx = (batch + full * copy).reshape(-1)
    ncopy = (jnp.max(copy) + 1).reshape(1)

    aff = as_rows(affinity)
    exp = as_rows(exposure)
    nlive = jnp.broadcast_to((lengths // BLOCK)[:, None], (members, BLOCK))
    limit = own_block(item_limit)
    duals = own_block(item_duals)

    own_d, other_d = gather_halves(duals)
    keep, send = iteration_kernel(False, groups, blocks, half, item_count)(
        gidx, sidx, ncopy, own_d, other_d, aff, exp, nlive)
    gradient = reduce_loads(keep, send) - limit

    own_g, other_g = gather_halves(gradient)
    keep, send, primal, sumsq = iteration_kernel(True, groups, blocks, half, item_count)(
        gidx, sidx, ncopy, own_d, other_d, own_g, other_g, aff, exp, nlive)
    scale = jnp.sqrt(sumsq[0:1, :] / item_count + 1e-6)
    duals = jnp.maximum(duals + 0.5 * gradient / scale, 0.0)

    gradient = reduce_loads(keep, send) - limit
    part = jnp.sum(gradient * gradient).reshape(1, 1)
    parts = lax.all_to_all(jnp.broadcast_to(part, (shard_size, 1)), "shard", 0, 0, tiled=True)
    scale = jnp.sqrt(jnp.sum(parts) / item_count + 1e-6)
    duals = jnp.maximum(duals + 0.5 * gradient / scale, 0.0)

    primal = primal.reshape(groups, blocks, SUB, BLOCK).transpose(0, 2, 1, 3).reshape(members, slots)
    return primal, duals[:own_rows].reshape(-1)


def solution(mesh):
    placed = (
        P(("grp", "shard"), None),
        P(("grp", "shard"), None),
        P(("grp", "shard"), None),
        P(("grp", "shard")),
        P("shard"),
        P("shard"),
    )

    def run(*args):
        return local(*args, grp_size=mesh.shape["grp"], shard_size=mesh.shape["shard"])

    return jax.shard_map(
        run,
        mesh=mesh,
        in_specs=placed,
        out_specs=(P(("grp", "shard"), None), P("shard")),
        check_vma=False,
    )
```

```python
import jax
import jax.numpy as jnp
from jax import lax
from jax.experimental import pallas as pl
from jax.experimental.pallas import tpu as pltpu
from jax.sharding import PartitionSpec as P

BLOCK = 128
BISECT = 16
SUB = 8
DEAD = -1e30

AXES = ("grp", "shard")


def pad8(n):
    return -(-n // SUB) * SUB


def iteration_kernel(second, groups, blocks, half, item_count):
    full = 2 * half
    members = groups * SUB
    group_rows = SUB * blocks
    part = groups // 2
    per_pass = part // BISECT
    assert per_pass * BISECT * 2 == groups
    f32 = jnp.float32

    def body(*refs):
        if second:
            (gidx, sidx, ncopy, own_d, other_d, own_g, other_g, aff, exp, nlive,
             keep, send, primal, sumsq, table, work_a, work_b, acc, lo, up) = refs
        else:
            (gidx, sidx, ncopy, own_d, other_d, aff, exp, nlive,
             keep, send, table, work_a, work_b, acc, lo, up) = refs
        works = (work_a, work_b)

        if second:
            def square(i, s):
                r = pl.multiple_of(i * SUB, SUB)
                a = own_g[pl.ds(r, SUB), :]
                b = other_g[pl.ds(r, SUB), :]
                return s + (a * a + b * b)

            s = lax.fori_loop(0, half // SUB, square, jnp.zeros((SUB, BLOCK), f32), unroll=8)
            total = jnp.sum(jnp.sum(s, axis=1, keepdims=True), axis=0, keepdims=True)
            total = jnp.broadcast_to(total, (SUB, BLOCK))
            sumsq[...] = total
            scale = jnp.sqrt(total / item_count + 1e-6)

            def fill_table(i, c):
                r = pl.multiple_of(i * SUB, SUB)
                for d, g, off in ((own_d, own_g, 0), (other_d, other_g, half)):
                    table[pl.ds(r + off, SUB), :] = jnp.maximum(
                        d[pl.ds(r, SUB), :] + 0.5 * g[pl.ds(r, SUB), :] / scale, 0.0)
                return c
        else:
            def fill_table(i, c):
                r = pl.multiple_of(i * SUB, SUB)
                table[pl.ds(r, SUB), :] = own_d[pl.ds(r, SUB), :]
                table[pl.ds(r + half, SUB), :] = other_d[pl.ds(r, SUB), :]
                return c

        lax.fori_loop(0, half // SUB, fill_table, 0, unroll=8)

        n = ncopy[0]
        zero = jnp.zeros((SUB, BLOCK), f32)

        def clear(i, c):
            acc[pl.ds(pl.multiple_of(i * SUB, SUB), SUB), :] = zero
            return c

        lax.fori_loop(
            0, n, lambda t, c: lax.fori_loop(
                0, full // SUB, lambda i, c: clear(t * (full // SUB) + i, c), c, unroll=16), 0)

        def gather_steps(h, g):
            base = pl.multiple_of((h * part + g) * group_rows, group_rows)
            here = pl.multiple_of(g * group_rows, group_rows)
            work = works[h].at[pl.ds(here, group_rows), :]
            a_rows = aff.at[pl.ds(base, group_rows), :]
            e_rows = exp.at[pl.ds(base, group_rows), :]
            ids = gidx.at[pl.ds(base, group_rows)]
            mrows = pl.ds(pl.multiple_of((h * part + g) * SUB, SUB), SUB)
            live = nlive[mrows, :]
            peak = [jnp.full((SUB, BLOCK), DEAD, f32)]

            def step(b):
                for s in range(SUB):
                    work[pl.ds(b * SUB + s, 1), :] = table[pl.ds(ids[s * blocks + b], 1), :]
                rows = pl.ds(b * SUB, SUB)
                v = (a_rows[rows, :] - e_rows[rows, :] * work[rows, :]) * 2.0
                v = jnp.where(live > b, v, DEAD)
                work[rows, :] = v
                peak[0] = jnp.maximum(peak[0], v)

            def end():
                up[mrows, :] = peak[0]

            return [lambda b=b: step(b) for b in range(blocks)] + [end]

        def start_bisection(h):
            for g in range(part):
                rows = pl.ds((h * part + g) * SUB, SUB)
                up[rows, :] = jnp.broadcast_to(jnp.max(up[rows, :], axis=1, keepdims=True), (SUB, BLOCK))
                lo[rows, :] = zero

        def bisect_steps(h):
            def step(g):
                rows = pl.ds((h * part + g) * SUB, SUB)
                mid = (lo[rows, :] + up[rows, :]) * 0.5
                sums = [None, None]
                for b in range(blocks):
                    v = jnp.clip(works[h][pl.ds(g * group_rows + b * SUB, SUB), :] - mid, 0.0, 1.0)
                    sums[b % 2] = v if sums[b % 2] is None else sums[b % 2] + v
                fill = jnp.broadcast_to(jnp.sum(sums[0] + sums[1], axis=1, keepdims=True), (SUB, BLOCK))
                bigger = fill > 1.0
                lo[rows, :] = jnp.where(bigger, mid, lo[rows, :])
                up[rows, :] = jnp.where(bigger, up[rows, :], mid)

            return [lambda g=g: step(g) for g in range(part)]

        def scatter_steps(h, g):
            base = pl.multiple_of((h * part + g) * group_rows, group_rows)
            here = pl.multiple_of(g * group_rows, group_rows)
            work = works[h].at[pl.ds(here, group_rows), :]
            e_rows = exp.at[pl.ds(base, group_rows), :]
            ids = sidx.at[pl.ds(base, group_rows)]
            mrows = pl.ds(pl.multiple_of((h * part + g) * SUB, SUB), SUB)

            def allocate():
                th = up[mrows, :]
                live = nlive[mrows, :]
                for b in range(blocks):
                    rows = pl.ds(b * SUB, SUB)
                    x = jnp.where(live > b, jnp.clip(work[rows, :] - th, 0.0, 1.0), 0.0)
                    if second:
                        primal[pl.ds(base + b * SUB, SUB), :] = x
                    work[rows, :] = e_rows[rows, :] * x

            def add(s):
                where = [ids[s * blocks + b] for b in range(blocks)]
                sums = [acc[pl.ds(i, 1), :] + work[pl.ds(b * SUB + s, 1), :] for b, i in enumerate(where)]
                for i, v in zip(where, sums):
                    acc[pl.ds(i, 1), :] = v

            return [allocate] + [lambda s=s: add(s) for s in range(SUB)]

        def together(first, other):
            done = 0
            for k, f in enumerate(first):
                f()
                want = (k + 1) * len(other) // len(first)
                for o in other[done:want]:
                    o()
                done = want

        def run(steps):
            for f in steps:
                f()

        def loop(count, f):
            def trip(i, c):
                f(i)
                return c

            lax.fori_loop(0, count, trip, 0)

        def several(steps, h, p):
            return [f for k in range(per_pass) for f in steps(h, p * per_pass + k)]

        loop(part, lambda g: run(gather_steps(0, g)))
        start_bisection(0)
        loop(BISECT, lambda p: together(bisect_steps(0), several(gather_steps, 1, p)))
        start_bisection(1)
        loop(BISECT, lambda p: together(bisect_steps(1), several(scatter_steps, 0, p)))
        loop(part, lambda g: run(scatter_steps(1, g)))

        def finish(i, c):
            r = pl.multiple_of(i * SUB, SUB)
            keep[pl.ds(r, SUB), :] = acc[pl.ds(r, SUB), :]
            send[pl.ds(r, SUB), :] = acc[pl.ds(r + half, SUB), :]
            return c

        lax.fori_loop(0, half // SUB, finish, 0, unroll=8)

        def finish_copy(t, c):
            def more(i, c):
                r = pl.multiple_of(i * SUB, SUB)
                o = pl.multiple_of(t * full + r, SUB)
                keep[pl.ds(r, SUB), :] += acc[pl.ds(o, SUB), :]
                send[pl.ds(r, SUB), :] += acc[pl.ds(o + half, SUB), :]
                return c

            return lax.fori_loop(0, half // SUB, more, c, unroll=8)

        lax.fori_loop(1, n, finish_copy, 0)

    rows = members * blocks
    smem = pl.BlockSpec(memory_space=pltpu.SMEM)
    vmem = pl.BlockSpec(memory_space=pltpu.VMEM)
    outs = [jax.ShapeDtypeStruct((half, BLOCK), f32)] * 2
    if second:
        outs += [jax.ShapeDtypeStruct((rows, BLOCK), f32), jax.ShapeDtypeStruct((SUB, BLOCK), f32)]
    return pl.pallas_call(
        body,
        out_shape=outs,
        in_specs=[smem] * 3 + [vmem] * (7 if second else 5),
        out_specs=[vmem] * len(outs),
        scratch_shapes=[
            pltpu.VMEM((full, BLOCK), f32),
            pltpu.VMEM((rows // 2, BLOCK), f32),
            pltpu.VMEM((rows // 2, BLOCK), f32),
            pltpu.VMEM((blocks * full, BLOCK), f32),
            pltpu.VMEM((members, BLOCK), f32),
            pltpu.VMEM((members, BLOCK), f32),
        ],
        compiler_params=pltpu.CompilerParams(vmem_limit_bytes=44 << 20),
        name="iterate2" if second else "iterate1",
    )


def local(candidates, affinity, exposure, lengths, item_limit, item_duals, *, grp_size, shard_size):
    chips = shard_size // 2
    same_core = [[2 * p + c for p in range(chips)] for c in range(2)]
    swap = [(g * shard_size + s, g * shard_size + (s ^ 1)) for g in range(grp_size) for s in range(shard_size)]
    members, slots = affinity.shape
    blocks = slots // BLOCK
    groups = members // SUB
    own_items = item_limit.shape[0]
    item_count = own_items * shard_size
    own_rows = own_items // BLOCK
    padded = pad8(own_rows)
    half = chips * padded
    full = 2 * half
    core = lax.axis_index("shard") % 2

    def swap_cores(x):
        return lax.ppermute(x, AXES, swap)

    def as_rows(x):
        return x.reshape(groups, SUB, blocks, BLOCK).transpose(0, 2, 1, 3).reshape(-1, BLOCK)

    def own_block(x):
        return jnp.pad(x.reshape(own_rows, BLOCK), ((0, padded - own_rows), (0, 0)))

    def gather_halves(x):
        every = lax.all_to_all(
            jnp.broadcast_to(x[None], (chips, padded, BLOCK)), "shard", 0, 0,
            axis_index_groups=same_core, tiled=True).reshape(half, BLOCK)
        return every, swap_cores(every)

    def reduce_loads(keep, send):
        chip = keep + swap_cores(send)
        plane = lax.all_to_all(
            chip.reshape(chips, padded, BLOCK), "shard", 0, 0,
            axis_index_groups=same_core, tiled=True).sum(axis=0)
        shifted = [
            lax.ppermute(plane, "grp", [(g, (g + d) % grp_size) for g in range(grp_size)])
            for d in range(1, grp_size)
        ]
        return (plane + shifted[1]) + (shifted[0] + shifted[2])

    shard_of = candidates // own_rows
    gidx = (jnp.where(shard_of % 2 == core, 0, half) + (shard_of // 2) * padded + candidates % own_rows).reshape(-1)
    batch = gidx.reshape(-1, blocks)
    earlier = jnp.arange(blocks)[:, None] > jnp.arange(blocks)[None, :]
    copy = jnp.sum((batch[:, :, None] == batch[:, None, :]) & earlier, axis=2, dtype=jnp.int32)
    sidx = (batch + full * copy).reshape(-1)
    ncopy = (jnp.max(copy) + 1).reshape(1)

    aff = as_rows(affinity)
    exp = as_rows(exposure)
    nlive = jnp.broadcast_to((lengths // BLOCK)[:, None], (members, BLOCK))
    limit = own_block(item_limit)
    duals = own_block(item_duals)

    own_d, other_d = gather_halves(duals)
    keep, send = iteration_kernel(False, groups, blocks, half, item_count)(
        gidx, sidx, ncopy, own_d, other_d, aff, exp, nlive)
    gradient = reduce_loads(keep, send) - limit

    own_g, other_g = gather_halves(gradient)
    keep, send, primal, sumsq = iteration_kernel(True, groups, blocks, half, item_count)(
        gidx, sidx, ncopy, own_d, other_d, own_g, other_g, aff, exp, nlive)
    scale = jnp.sqrt(sumsq[0:1, :] / item_count + 1e-6)
    duals = jnp.maximum(duals + 0.5 * gradient / scale, 0.0)

    gradient = reduce_loads(keep, send) - limit
    part = jnp.sum(gradient * gradient).reshape(1, 1)
    parts = lax.all_to_all(jnp.broadcast_to(part, (shard_size, 1)), "shard", 0, 0, tiled=True)
    scale = jnp.sqrt(jnp.sum(parts) / item_count + 1e-6)
    duals = jnp.maximum(duals + 0.5 * gradient / scale, 0.0)

    primal = primal.reshape(groups, blocks, SUB, BLOCK).transpose(0, 2, 1, 3).reshape(members, slots)
    return primal, duals[:own_rows].reshape(-1)


def solution(mesh):
    placed = (
        P(("grp", "shard"), None),
        P(("grp", "shard"), None),
        P(("grp", "shard"), None),
        P(("grp", "shard")),
        P("shard"),
        P("shard"),
    )

    def run(*args):
        return local(*args, grp_size=mesh.shape["grp"], shard_size=mesh.shape["shard"])

    return jax.shard_map(
        run,
        mesh=mesh,
        in_specs=placed,
        out_specs=(P(("grp", "shard"), None), P("shard")),
        check_vma=False,
    )
```

```python
import jax
import jax.numpy as jnp
from jax import lax
from jax.experimental import pallas as pl
from jax.experimental.pallas import tpu as pltpu
from jax.sharding import PartitionSpec as P

BLOCK = 128
BISECT = 16
SUB = 8
DEAD = -1e30

AXES = ("grp", "shard")


def pad8(n):
    return -(-n // SUB) * SUB


def iteration_kernel(second, groups, blocks, half, item_count):
    full = 2 * half
    members = groups * SUB
    group_rows = SUB * blocks
    rows_all = groups * group_rows
    part = groups // 2
    quarter = part // 2
    part_rows = part * group_rows
    assert quarter * 4 == groups and part == BISECT and blocks % 2 == 0
    pieces = 4
    f32 = jnp.float32

    def body(*refs):
        if second:
            (gidx_in, sidx_in, ncopy, own_d, other_d, own_g, other_g, aff_in, exp_in, nlive,
             keep, send, primal_out, sumsq,
             table, work_a, work_b, acc, lo, up, peaks, sums, aff, exp, gidx, sidx, sem_in, sem_id,
             primal, sem_out) = refs
        else:
            (gidx_in, sidx_in, ncopy, own_d, other_d, aff_in, exp_in, nlive,
             keep, send,
             table, work_a, work_b, acc, lo, up, peaks, sums, aff, exp, gidx, sidx, sem_in, sem_id) = refs
        works = (work_a, work_b)

        ids_in = [pltpu.make_async_copy(src, dst, sem_id.at[k])
                  for k, (src, dst) in enumerate(((gidx_in, gidx), (sidx_in, sidx)))]
        size = part_rows // pieces
        spans = [(k * size, size) for k in range(pieces)] + [(part_rows, part_rows)]
        loads = [[pltpu.make_async_copy(src.at[pl.ds(r, n), :], dst.at[pl.ds(r, n), :], sem_in.at[k, j])
                  for j, (src, dst) in enumerate(((aff_in, aff), (exp_in, exp)))]
                 for k, (r, n) in enumerate(spans)]
        ids_in[0].start()
        for pair in loads:
            for load in pair:
                load.start()
        ids_in[1].start()

        if second:
            def square(i, s):
                r = pl.multiple_of(i * SUB, SUB)
                a = own_g[pl.ds(r, SUB), :]
                b = other_g[pl.ds(r, SUB), :]
                return s + (a * a + b * b)

            s = lax.fori_loop(0, half // SUB, square, jnp.zeros((SUB, BLOCK), f32), unroll=8)
            total = jnp.sum(jnp.sum(s, axis=1, keepdims=True), axis=0, keepdims=True)
            total = jnp.broadcast_to(total, (SUB, BLOCK))
            sumsq[...] = total
            scale = jnp.sqrt(total / item_count + 1e-6)

            def fill_table(i, c):
                r = pl.multiple_of(i * SUB, SUB)
                for d, g, off in ((own_d, own_g, 0), (other_d, other_g, half)):
                    table[pl.ds(r + off, SUB), :] = jnp.maximum(
                        d[pl.ds(r, SUB), :] + 0.5 * g[pl.ds(r, SUB), :] / scale, 0.0)
                return c
        else:
            def fill_table(i, c):
                r = pl.multiple_of(i * SUB, SUB)
                table[pl.ds(r, SUB), :] = own_d[pl.ds(r, SUB), :]
                table[pl.ds(r + half, SUB), :] = other_d[pl.ds(r, SUB), :]
                return c

        lax.fori_loop(0, half // SUB, fill_table, 0, unroll=8)

        n = ncopy[0]
        zero = jnp.zeros((SUB, BLOCK), f32)
        dead = jnp.full((SUB, BLOCK), DEAD, f32)
        vregs = full // SUB
        per_step = 2 * vregs // (2 * BISECT)
        assert per_step * BISECT == vregs

        def clear(i, c):
            acc[pl.ds(pl.multiple_of(i * SUB, SUB), SUB), :] = zero
            return c

        lax.fori_loop(2 * vregs // 16, n * vregs // 16, lambda i, c: [clear(16 * i + j, c) for j in range(16)][-1], 0)

        def clear_some(k):
            some = acc.at[pl.ds(pl.multiple_of(k * (per_step * SUB), SUB), per_step * SUB), :]
            for i in range(per_step):
                some[pl.ds(i * SUB, SUB), :] = zero

        def loop(first, last, f):
            def trip(i, c):
                f(i)
                return c

            lax.fori_loop(first, last, trip, 0)

        def picked(ids, j, g):
            return ids.at[pl.ds(j * groups, rows_all - j * groups)][g]

        def gather(h, g, first, count):
            rows = (h * part + g) * group_rows
            where = pl.multiple_of(rows + first * SUB, SUB)
            here = pl.multiple_of(g * group_rows + first * SUB, SUB)
            work = works[h].at[pl.ds(here, count * SUB), :]
            a_rows = aff.at[pl.ds(where, count * SUB), :]
            e_rows = exp.at[pl.ds(where, count * SUB), :]
            mrows = pl.ds(pl.multiple_of((h * part + g) * SUB, SUB), SUB)
            live = nlive[mrows, :] - first
            peak = peaks[mrows, :]
            for b in range(count):
                for s in range(SUB):
                    work[pl.ds(b * SUB + s, 1), :] = table[pl.ds(picked(gidx, s * blocks + b, h * part + g + first * groups), 1), :]
                now = pl.ds(b * SUB, SUB)
                v = (a_rows[now, :] - e_rows[now, :] * work[now, :]) * 2.0
                v = jnp.where(live > b, v, DEAD)
                work[now, :] = v
                peak = jnp.maximum(peak, v)
            peaks[mrows, :] = peak

        def start_bisection(h):
            for g in range(part):
                rows = pl.ds((h * part + g) * SUB, SUB)
                up[rows, :] = jnp.broadcast_to(jnp.max(peaks[rows, :], axis=1, keepdims=True), (SUB, BLOCK))
                lo[rows, :] = zero

        def fill_sums(h, q, *only):
            work = works[h].at[pl.ds(pl.multiple_of(q * (quarter * group_rows), SUB), quarter * group_rows), :]
            m0 = pl.multiple_of((h * part + q * quarter) * SUB, SUB)
            s0 = pl.multiple_of(q * (quarter * SUB), SUB)
            for g in only or range(quarter):
                rows = pl.ds(m0 + g * SUB, SUB)
                mid = (lo[rows, :] + up[rows, :]) * 0.5
                a = [None, None]
                for b in range(blocks):
                    v = jnp.clip(work[pl.ds(g * group_rows + b * SUB, SUB), :] - mid, 0.0, 1.0)
                    a[b % 2] = v if a[b % 2] is None else a[b % 2] + v
                sums[pl.ds(s0 + g * SUB, SUB), :] = a[0] + a[1]

        def lane_sums(q):
            s0 = pl.multiple_of(q * (quarter * SUB), SUB)
            return [jnp.sum(sums[pl.ds(s0 + g * SUB, SUB), :], axis=1, keepdims=True) for g in range(quarter)]

        def decide(h, q, fills):
            m0 = pl.multiple_of((h * part + q * quarter) * SUB, SUB)
            for g in range(quarter):
                rows = pl.ds(m0 + g * SUB, SUB)
                bigger = jnp.broadcast_to(fills[g], (SUB, BLOCK)) > 1.0
                low = lo[rows, :]
                high = up[rows, :]
                mid = (low + high) * 0.5
                lo[rows, :] = jnp.where(bigger, mid, low)
                up[rows, :] = jnp.where(bigger, high, mid)

        def bisect(h, beside):
            fill_sums(h, 0)

            def half_step(k):
                q = k % 2
                fills = lane_sums(q)
                steps = beside(k // 2, q)
                for g in range(quarter):
                    fill_sums(h, 1 - q, g)
                    for at, step in steps:
                        if at == g:
                            step()
                decide(h, q, fills)

            loop(0, 2 * BISECT, half_step)

        def allocate(h, g):
            rows = pl.multiple_of((h * part + g) * group_rows, SUB)
            here = pl.multiple_of(g * group_rows, SUB)
            mrows = pl.ds(pl.multiple_of((h * part + g) * SUB, SUB), SUB)
            th = up[mrows, :]
            live = nlive[mrows, :]
            for b in range(blocks):
                now = pl.ds(here + b * SUB, SUB)
                x = jnp.where(live > b, jnp.clip(works[h][now, :] - th, 0.0, 1.0), 0.0)
                if second:
                    primal[pl.ds(rows + b * SUB, SUB), :] = x
                works[h][now, :] = exp[pl.ds(rows + b * SUB, SUB), :] * x

        def scatter(h, g, first, count):
            here = g * group_rows + first
            work = works[h]
            for s in range(count):
                where = [picked(sidx, s * blocks + b, h * part + g + first * blocks * groups) for b in range(blocks)]
                added = [acc[pl.ds(i, 1), :] + work[pl.ds(here + b * SUB + s, 1), :] for b, i in enumerate(where)]
                for i, v in zip(where, added):
                    acc[pl.ds(i, 1), :] = v

        for g in range(groups):
            peaks[pl.ds(g * SUB, SUB), :] = dead
        ids_in[0].wait()
        for k in range(pieces):
            for load in loads[k]:
                load.wait()
            loop(k * (part // pieces), (k + 1) * (part // pieces), lambda g: gather(0, g, 0, blocks))
        start_bisection(0)
        for load in loads[pieces]:
            load.wait()
        bisect(0, lambda g, q: [(quarter - 1, lambda: gather(1, g, q * (blocks // 2), blocks // 2)),
                                (quarter - 1, lambda: clear_some(2 * g + q))])

        start_bisection(1)
        loop(0, part, lambda g: allocate(0, g))
        if second:
            stores = [pltpu.make_async_copy(
                primal.at[pl.ds(h * part_rows, part_rows), :],
                primal_out.at[pl.ds(h * part_rows, part_rows), :], sem_out.at[h]) for h in range(2)]
            stores[0].start()
        ids_in[1].wait()
        bisect(1, lambda g, q: [(2 * m, lambda m=m: scatter(0, g, q * (SUB // 2) + m, 1)) for m in range(SUB // 2)])
        loop(0, part, lambda g: allocate(1, g))
        if second:
            stores[1].start()
        loop(0, part, lambda g: scatter(1, g, 0, SUB))

        def finish(i, c):
            r = pl.multiple_of(i * SUB, SUB)
            for out, o in ((keep, 0), (send, half)):
                out[pl.ds(r, SUB), :] = acc[pl.ds(r + o, SUB), :] + acc[pl.ds(r + (full + o), SUB), :]
            return c

        lax.fori_loop(0, half // SUB, finish, 0, unroll=8)

        def finish_copy(t, c):
            def more(i, c):
                r = pl.multiple_of(i * SUB, SUB)
                a = pl.multiple_of(t * full + r, SUB)
                for out, o in ((keep, 0), (send, half)):
                    out[pl.ds(r, SUB), :] += acc[pl.ds(a + o, SUB), :]
                return c

            return lax.fori_loop(0, half // SUB, more, c, unroll=8)

        lax.fori_loop(2, n, finish_copy, 0)
        if second:
            for store in stores:
                store.wait()

    smem = pl.BlockSpec(memory_space=pltpu.SMEM)
    vmem = pl.BlockSpec(memory_space=pltpu.VMEM)
    left = pl.BlockSpec(memory_space=pltpu.HBM)
    outs = [jax.ShapeDtypeStruct((half, BLOCK), f32)] * 2
    out_specs = [vmem] * 2
    scratch = [
        pltpu.VMEM((full, BLOCK), f32),
        pltpu.VMEM((part_rows, BLOCK), f32),
        pltpu.VMEM((part_rows, BLOCK), f32),
        pltpu.VMEM((blocks * full, BLOCK), f32),
        pltpu.VMEM((members, BLOCK), f32),
        pltpu.VMEM((members, BLOCK), f32),
        pltpu.VMEM((members, BLOCK), f32),
        pltpu.VMEM((part * SUB, BLOCK), f32),
        pltpu.VMEM((rows_all, BLOCK), f32),
        pltpu.VMEM((rows_all, BLOCK), f32),
        pltpu.SMEM((rows_all,), jnp.int32),
        pltpu.SMEM((rows_all,), jnp.int32),
        pltpu.SemaphoreType.DMA((pieces + 1, 2)),
        pltpu.SemaphoreType.DMA((2,)),
    ]
    if second:
        outs += [jax.ShapeDtypeStruct((rows_all, BLOCK), f32), jax.ShapeDtypeStruct((SUB, BLOCK), f32)]
        out_specs += [left, vmem]
        scratch += [pltpu.VMEM((rows_all, BLOCK), f32), pltpu.SemaphoreType.DMA((2,))]
    tables = [vmem] * (4 if second else 2)
    call = pl.pallas_call(
        body,
        out_shape=outs,
        in_specs=[left, left, smem] + tables + [left, left, vmem],
        out_specs=out_specs,
        scratch_shapes=scratch,
        compiler_params=pltpu.CompilerParams(vmem_limit_bytes=48 << 20),
        name="iterate2" if second else "iterate1",
    )

    def run(gidx, sidx, ncopy, *rest):
        *tables, aff, exp, nlive = rest
        aff, exp = (pltpu.with_memory_space_constraint(x, pltpu.HBM) for x in (aff, exp))
        return call(gidx, sidx, ncopy, *tables, aff, exp, nlive)

    return run


def vmem_call(body, name, *outs):
    spec = pl.BlockSpec(memory_space=pltpu.VMEM)
    return pl.pallas_call(
        body,
        out_shape=[jax.ShapeDtypeStruct(shape, jnp.float32) for shape in outs],
        out_specs=[spec] * len(outs),
        compiler_params=pltpu.CompilerParams(vmem_limit_bytes=4 << 20),
        name=name,
    )


def spread_duals(x, chips, padded, core):
    own_rows = x.shape[0]

    def body(x, core, every):
        for p in range(chips):
            every[p, pl.ds(0, own_rows), :] = x[...]
            every[p, pl.ds(own_rows, padded - own_rows), :] = jnp.zeros((padded - own_rows, BLOCK), jnp.float32)

    return vmem_call(body, "spread_duals", (chips, padded, BLOCK))(
        x, jnp.full((SUB, BLOCK), core, jnp.int32))[0]


def sum_chips(x):
    def body(x, out):
        out[...] = jnp.sum(x[...], axis=0)

    return vmem_call(body, "sum_chips", x.shape[1:])(x)[0]


def gradient_of(plane, shifted, limit, gradient):
    own_rows = limit.shape[0]
    one, two, three = shifted
    gradient[...] = (plane[...] + two[...]) + (one[...] + three[...])
    gradient[pl.ds(0, own_rows), :] = gradient[pl.ds(0, own_rows), :] - limit[...]


def spread_gradient(plane, shifted, limit, chips):
    def body(plane, one, two, three, limit, gradient, every):
        gradient_of(plane, (one, two, three), limit, gradient)
        for p in range(chips):
            every[p] = gradient[...]

    return vmem_call(body, "spread_gradient", plane.shape, (chips, *plane.shape))(plane, *shifted, limit)


def last_gradient(plane, shifted, limit, shards):
    def body(plane, one, two, three, limit, gradient, parts):
        gradient_of(plane, (one, two, three), limit, gradient)
        g = gradient[...]
        part = jnp.sum(jnp.sum(g * g, axis=0, keepdims=True), axis=1, keepdims=True)
        parts[...] = jnp.broadcast_to(part[None], parts.shape)

    return vmem_call(body, "last_gradient", plane.shape, (shards, 1, BLOCK))(plane, *shifted, limit)


def last_duals(duals, first, sumsq, second, parts, item_count):
    own_rows = duals.shape[0]

    def body(duals, first, sumsq, second, parts, out):
        own = pl.ds(0, own_rows)
        scale = jnp.sqrt(sumsq[0:1, :] / item_count + 1e-6)
        lam = jnp.maximum(duals[...] + 0.5 * first[own, :] / scale, 0.0)
        scale = jnp.sqrt(jnp.sum(parts[...], axis=0) / item_count + 1e-6)
        out[...] = jnp.maximum(lam + 0.5 * second[own, :] / scale, 0.0)

    return vmem_call(body, "last_duals", duals.shape)(duals, first, sumsq, second, parts)[0]


def local(candidates, affinity, exposure, lengths, item_limit, item_duals, *, grp_size, shard_size):
    chips = shard_size // 2
    same_core = [[2 * p + c for p in range(chips)] for c in range(2)]
    swap = [(g * shard_size + s, g * shard_size + (s ^ 1)) for g in range(grp_size) for s in range(shard_size)]
    members, slots = affinity.shape
    blocks = slots // BLOCK
    groups = members // SUB
    own_items = item_limit.shape[0]
    item_count = own_items * shard_size
    own_rows = own_items // BLOCK
    padded = pad8(own_rows)
    half = chips * padded
    full = 2 * half
    core = lax.axis_index("shard") % 2

    def swap_cores(x):
        return lax.ppermute(x, AXES, swap)

    def as_rows(x):
        return x.reshape(groups, SUB, blocks, BLOCK).transpose(0, 2, 1, 3).reshape(-1, BLOCK)

    def gather_halves(every):
        every = lax.all_to_all(
            every, "shard", 0, 0, axis_index_groups=same_core, tiled=True).reshape(half, BLOCK)
        return every, swap_cores(every)

    def reduce_loads(keep, send):
        chip = keep + swap_cores(send)
        plane = sum_chips(lax.all_to_all(
            chip.reshape(chips, padded, BLOCK), "shard", 0, 0,
            axis_index_groups=same_core, tiled=True))
        return plane, [
            lax.ppermute(plane, "grp", [(g, (g + d) % grp_size) for g in range(grp_size)])
            for d in range(1, grp_size)
        ]

    shard_of = candidates // own_rows
    gidx = (jnp.where(shard_of % 2 == core, 0, half) + (shard_of // 2) * padded + candidates % own_rows).reshape(-1)
    batch = gidx.reshape(-1, blocks)
    earlier = jnp.arange(blocks)[:, None] > jnp.arange(blocks)[None, :]
    copy = jnp.sum((batch[:, :, None] == batch[:, None, :]) & earlier, axis=2, dtype=jnp.int32)
    sidx = (batch + full * copy).reshape(groups, -1).T.reshape(-1)
    gidx = gidx.reshape(groups, -1).T.reshape(-1)
    ncopy = (jnp.max(copy) + 1).reshape(1)

    aff = as_rows(affinity)
    exp = as_rows(exposure)
    nlive = jnp.broadcast_to((lengths // BLOCK)[:, None], (members, BLOCK))
    limit = item_limit.reshape(own_rows, BLOCK)
    duals = item_duals.reshape(own_rows, BLOCK)

    own_d, other_d = gather_halves(spread_duals(duals, chips, padded, core))
    keep, send = iteration_kernel(False, groups, blocks, half, item_count)(
        gidx, sidx, ncopy, own_d, other_d, aff, exp, nlive)
    first, every = spread_gradient(*reduce_loads(keep, send), limit, chips)

    own_g, other_g = gather_halves(every)
    keep, send, primal, sumsq = iteration_kernel(True, groups, blocks, half, item_count)(
        gidx, sidx, ncopy, own_d, other_d, own_g, other_g, aff, exp, nlive)
    second, parts = last_gradient(*reduce_loads(keep, send), limit, shard_size)
    parts = lax.all_to_all(parts, "shard", 0, 0, tiled=True)
    duals = last_duals(duals, first, sumsq, second, parts, item_count)

    primal = primal.reshape(groups, blocks, SUB, BLOCK).transpose(0, 2, 1, 3).reshape(members, slots)
    return primal, duals.reshape(-1)


def solution(mesh):
    placed = (
        P(("grp", "shard"), None),
        P(("grp", "shard"), None),
        P(("grp", "shard"), None),
        P(("grp", "shard")),
        P("shard"),
        P("shard"),
    )

    def run(*args):
        return local(*args, grp_size=mesh.shape["grp"], shard_size=mesh.shape["shard"])

    return jax.shard_map(
        run,
        mesh=mesh,
        in_specs=placed,
        out_specs=(P(("grp", "shard"), None), P("shard")),
        check_vma=False,
    )
```

```python
import jax
import jax.numpy as jnp
from jax import lax
from jax.experimental import pallas as pl
from jax.experimental.pallas import tpu as pltpu
from jax.sharding import PartitionSpec as P

BLOCK = 128
BISECT = 16
SUB = 8
DEAD = -1e30

AXES = ("grp", "shard")


def iteration_kernel(second, groups, blocks, half, item_count):
    full = 2 * half
    members = groups * SUB
    group_rows = SUB * blocks
    rows_all = groups * group_rows
    part = groups // 2
    quarter = part // 2
    part_rows = part * group_rows
    assert quarter * 4 == groups and part == BISECT and blocks % 2 == 0
    pieces = 4
    f32 = jnp.float32

    def body(*refs):
        if second:
            (gidx_in, sidx_in, ncopy, own_d, other_d, own_g, other_g, aff_in, exp_in, nlive,
             keep, send, primal_out, sumsq,
             table, work_a, work_b, acc, lo, up, peaks, sums, aff, exp, gidx, sidx, sem_in, sem_id,
             primal, sem_out) = refs
        else:
            (gidx_in, sidx_in, ncopy, own_d, other_d, aff_in, exp_in, nlive,
             keep, send,
             table, work_a, work_b, acc, lo, up, peaks, sums, aff, exp, gidx, sidx, sem_in, sem_id) = refs
        works = (work_a, work_b)

        ids_in = [pltpu.make_async_copy(src, dst, sem_id.at[k])
                  for k, (src, dst) in enumerate(((gidx_in, gidx), (sidx_in, sidx)))]
        size = part_rows // pieces
        spans = [(k * size, size) for k in range(pieces)] + [(part_rows, part_rows)]
        loads = [[pltpu.make_async_copy(src.at[pl.ds(r, n), :], dst.at[pl.ds(r, n), :], sem_in.at[k, j])
                  for j, (src, dst) in enumerate(((aff_in, aff), (exp_in, exp)))]
                 for k, (r, n) in enumerate(spans)]
        ids_in[0].start()
        for pair in loads:
            for load in pair:
                load.start()
        ids_in[1].start()

        if second:
            def square(i, s):
                r = pl.multiple_of(i * SUB, SUB)
                a = own_g[pl.ds(r, SUB), :]
                b = other_g[pl.ds(r, SUB), :]
                return s + (a * a + b * b)

            s = lax.fori_loop(0, half // SUB, square, jnp.zeros((SUB, BLOCK), f32), unroll=8)
            total = jnp.sum(jnp.sum(s, axis=1, keepdims=True), axis=0, keepdims=True)
            total = jnp.broadcast_to(total, (SUB, BLOCK))
            sumsq[...] = total
            scale = jnp.sqrt(total / item_count + 1e-6)

            def fill_table(i, c):
                r = pl.multiple_of(i * SUB, SUB)
                for d, g, off in ((own_d, own_g, 0), (other_d, other_g, half)):
                    table[pl.ds(r + off, SUB), :] = jnp.maximum(
                        d[pl.ds(r, SUB), :] + 0.5 * g[pl.ds(r, SUB), :] / scale, 0.0)
                return c
        else:
            def fill_table(i, c):
                r = pl.multiple_of(i * SUB, SUB)
                table[pl.ds(r, SUB), :] = own_d[pl.ds(r, SUB), :]
                table[pl.ds(r + half, SUB), :] = other_d[pl.ds(r, SUB), :]
                return c

        lax.fori_loop(0, half // SUB, fill_table, 0, unroll=8)

        n = ncopy[0]
        zero = jnp.zeros((SUB, BLOCK), f32)
        dead = jnp.full((SUB, BLOCK), DEAD, f32)
        vregs = full // SUB
        per_step = 2 * vregs // (2 * BISECT)
        assert per_step * BISECT == vregs

        def clear(i, c):
            acc[pl.ds(pl.multiple_of(i * SUB, SUB), SUB), :] = zero
            return c

        lax.fori_loop(2 * vregs // 16, n * vregs // 16, lambda i, c: [clear(16 * i + j, c) for j in range(16)][-1], 0)

        def clear_some(k):
            some = acc.at[pl.ds(pl.multiple_of(k * (per_step * SUB), SUB), per_step * SUB), :]
            for i in range(per_step):
                some[pl.ds(i * SUB, SUB), :] = zero

        def loop(first, last, f):
            def trip(i, c):
                f(i)
                return c

            lax.fori_loop(first, last, trip, 0)

        def picked(ids, j, g):
            return ids.at[pl.ds(j * groups, rows_all - j * groups)][g]

        def gather(h, g, first, count):
            rows = (h * part + g) * group_rows
            where = pl.multiple_of(rows + first * SUB, SUB)
            here = pl.multiple_of(g * group_rows + first * SUB, SUB)
            work = works[h].at[pl.ds(here, count * SUB), :]
            a_rows = aff.at[pl.ds(where, count * SUB), :]
            e_rows = exp.at[pl.ds(where, count * SUB), :]
            mrows = pl.ds(pl.multiple_of((h * part + g) * SUB, SUB), SUB)
            live = nlive[mrows, :] - first
            peak = peaks[mrows, :]
            for b in range(count):
                for s in range(SUB):
                    work[pl.ds(b * SUB + s, 1), :] = table[pl.ds(picked(gidx, s * blocks + b, h * part + g + first * groups), 1), :]
                now = pl.ds(b * SUB, SUB)
                v = (a_rows[now, :] - e_rows[now, :] * work[now, :]) * 2.0
                v = jnp.where(live > b, v, DEAD)
                work[now, :] = v
                peak = jnp.maximum(peak, v)
            peaks[mrows, :] = peak

        def start_bisection(h):
            for g in range(part):
                rows = pl.ds((h * part + g) * SUB, SUB)
                up[rows, :] = jnp.broadcast_to(jnp.max(peaks[rows, :], axis=1, keepdims=True), (SUB, BLOCK))
                lo[rows, :] = zero

        def fill_sums(h, q, *only):
            work = works[h].at[pl.ds(pl.multiple_of(q * (quarter * group_rows), SUB), quarter * group_rows), :]
            m0 = pl.multiple_of((h * part + q * quarter) * SUB, SUB)
            s0 = pl.multiple_of(q * (quarter * SUB), SUB)
            for g in only or range(quarter):
                rows = pl.ds(m0 + g * SUB, SUB)
                mid = (lo[rows, :] + up[rows, :]) * 0.5
                a = [None, None]
                for b in range(blocks):
                    v = jnp.clip(work[pl.ds(g * group_rows + b * SUB, SUB), :] - mid, 0.0, 1.0)
                    a[b % 2] = v if a[b % 2] is None else a[b % 2] + v
                sums[pl.ds(s0 + g * SUB, SUB), :] = a[0] + a[1]

        def lane_sums(q):
            s0 = pl.multiple_of(q * (quarter * SUB), SUB)
            return [jnp.sum(sums[pl.ds(s0 + g * SUB, SUB), :], axis=1, keepdims=True) for g in range(quarter)]

        def decide(h, q, fills):
            m0 = pl.multiple_of((h * part + q * quarter) * SUB, SUB)
            for g in range(quarter):
                rows = pl.ds(m0 + g * SUB, SUB)
                bigger = jnp.broadcast_to(fills[g], (SUB, BLOCK)) > 1.0
                low = lo[rows, :]
                high = up[rows, :]
                mid = (low + high) * 0.5
                lo[rows, :] = jnp.where(bigger, mid, low)
                up[rows, :] = jnp.where(bigger, high, mid)

        def bisect(h, beside):
            fill_sums(h, 0)

            def half_step(k):
                q = k % 2
                fills = lane_sums(q)
                steps = beside(k // 2, q)
                for g in range(quarter):
                    fill_sums(h, 1 - q, g)
                    for at, step in steps:
                        if at == g:
                            step()
                decide(h, q, fills)

            loop(0, 2 * BISECT, half_step)

        def allocate(h, g):
            rows = pl.multiple_of((h * part + g) * group_rows, SUB)
            here = pl.multiple_of(g * group_rows, SUB)
            mrows = pl.ds(pl.multiple_of((h * part + g) * SUB, SUB), SUB)
            th = up[mrows, :]
            live = nlive[mrows, :]
            for b in range(blocks):
                now = pl.ds(here + b * SUB, SUB)
                x = jnp.where(live > b, jnp.clip(works[h][now, :] - th, 0.0, 1.0), 0.0)
                if second:
                    primal[pl.ds(rows + b * SUB, SUB), :] = x
                works[h][now, :] = exp[pl.ds(rows + b * SUB, SUB), :] * x

        def scatter(h, g, first, count):
            here = g * group_rows + first
            work = works[h]
            for s in range(count):
                where = [picked(sidx, s * blocks + b, h * part + g + first * blocks * groups) for b in range(blocks)]
                added = [acc[pl.ds(i, 1), :] + work[pl.ds(here + b * SUB + s, 1), :] for b, i in enumerate(where)]
                for i, v in zip(where, added):
                    acc[pl.ds(i, 1), :] = v

        for g in range(groups):
            peaks[pl.ds(g * SUB, SUB), :] = dead
        ids_in[0].wait()
        for k in range(pieces):
            for load in loads[k]:
                load.wait()
            loop(k * (part // pieces), (k + 1) * (part // pieces), lambda g: gather(0, g, 0, blocks))
        start_bisection(0)
        for load in loads[pieces]:
            load.wait()
        bisect(0, lambda g, q: [(quarter - 1, lambda: gather(1, g, q * (blocks // 2), blocks // 2)),
                                (quarter - 1, lambda: clear_some(2 * g + q))])

        start_bisection(1)
        loop(0, part, lambda g: allocate(0, g))
        if second:
            stores = [pltpu.make_async_copy(
                primal.at[pl.ds(h * part_rows, part_rows), :],
                primal_out.at[pl.ds(h * part_rows, part_rows), :], sem_out.at[h]) for h in range(2)]
            stores[0].start()
        ids_in[1].wait()
        bisect(1, lambda g, q: [(2 * m, lambda m=m: scatter(0, g, q * (SUB // 2) + m, 1)) for m in range(SUB // 2)])
        loop(0, part, lambda g: allocate(1, g))
        if second:
            stores[1].start()
        loop(0, part, lambda g: scatter(1, g, 0, SUB))

        def finish(i, c):
            r = pl.multiple_of(i * SUB, SUB)
            for out, o in ((keep, 0), (send, half)):
                out[pl.ds(r, SUB), :] = acc[pl.ds(r + o, SUB), :] + acc[pl.ds(r + (full + o), SUB), :]
            return c

        lax.fori_loop(0, half // SUB, finish, 0, unroll=8)

        def finish_copy(t, c):
            def more(i, c):
                r = pl.multiple_of(i * SUB, SUB)
                a = pl.multiple_of(t * full + r, SUB)
                for out, o in ((keep, 0), (send, half)):
                    out[pl.ds(r, SUB), :] += acc[pl.ds(a + o, SUB), :]
                return c

            return lax.fori_loop(0, half // SUB, more, c, unroll=8)

        lax.fori_loop(2, n, finish_copy, 0)
        if second:
            for store in stores:
                store.wait()

    smem = pl.BlockSpec(memory_space=pltpu.SMEM)
    vmem = pl.BlockSpec(memory_space=pltpu.VMEM)
    left = pl.BlockSpec(memory_space=pltpu.HBM)
    outs = [jax.ShapeDtypeStruct((half, BLOCK), f32)] * 2
    out_specs = [vmem] * 2
    scratch = [
        pltpu.VMEM((full, BLOCK), f32),
        pltpu.VMEM((part_rows, BLOCK), f32),
        pltpu.VMEM((part_rows, BLOCK), f32),
        pltpu.VMEM((blocks * full, BLOCK), f32),
        pltpu.VMEM((members, BLOCK), f32),
        pltpu.VMEM((members, BLOCK), f32),
        pltpu.VMEM((members, BLOCK), f32),
        pltpu.VMEM((part * SUB, BLOCK), f32),
        pltpu.VMEM((rows_all, BLOCK), f32),
        pltpu.VMEM((rows_all, BLOCK), f32),
        pltpu.SMEM((rows_all,), jnp.int32),
        pltpu.SMEM((rows_all,), jnp.int32),
        pltpu.SemaphoreType.DMA((pieces + 1, 2)),
        pltpu.SemaphoreType.DMA((2,)),
    ]
    if second:
        outs += [jax.ShapeDtypeStruct((rows_all, BLOCK), f32), jax.ShapeDtypeStruct((SUB, BLOCK), f32)]
        out_specs += [left, vmem]
        scratch += [pltpu.VMEM((rows_all, BLOCK), f32), pltpu.SemaphoreType.DMA((2,))]
    tables = [vmem] * (4 if second else 2)
    call = pl.pallas_call(
        body,
        out_shape=outs,
        in_specs=[left, left, smem] + tables + [left, left, vmem],
        out_specs=out_specs,
        scratch_shapes=scratch,
        compiler_params=pltpu.CompilerParams(vmem_limit_bytes=48 << 20),
        name="iterate2" if second else "iterate1",
    )

    def run(gidx, sidx, ncopy, *rest):
        *tables, aff, exp, nlive = rest
        aff, exp = (pltpu.with_memory_space_constraint(x, pltpu.HBM) for x in (aff, exp))
        return call(gidx, sidx, ncopy, *tables, aff, exp, nlive)

    return run


def vmem_call(body, name, *outs):
    spec = pl.BlockSpec(memory_space=pltpu.VMEM)
    return pl.pallas_call(
        body,
        out_shape=[jax.ShapeDtypeStruct(shape, jnp.float32) for shape in outs],
        out_specs=[spec] * len(outs),
        compiler_params=pltpu.CompilerParams(vmem_limit_bytes=4 << 20),
        name=name,
    )


def spread_duals(x, chips, core):
    own_rows = x.shape[0]

    def body(x, core, every):
        for p in range(chips):
            every[pl.ds(p * own_rows, own_rows), :] = x[...]

    return vmem_call(body, "spread_duals", (chips * own_rows, BLOCK))(
        x, jnp.full((SUB, BLOCK), core, jnp.int32))[0]


def sum_chips(x, chips):
    own_rows = x.shape[0] // chips

    def body(x, out):
        parts = [x[pl.ds(p * own_rows, own_rows), :] for p in range(chips)]
        while len(parts) > 1:
            parts = [a + b for a, b in zip(parts[::2], parts[1::2])]
        out[...] = parts[0]

    return vmem_call(body, "sum_chips", (own_rows, BLOCK))(x)[0]


def gradient_of(plane, shifted, limit):
    one, two, three = shifted
    return ((plane[...] + two[...]) + (one[...] + three[...])) - limit[...]


def spread_gradient(plane, shifted, limit, chips):
    own_rows = plane.shape[0]

    def body(plane, one, two, three, limit, gradient, every):
        g = gradient_of(plane, (one, two, three), limit)
        gradient[...] = g
        for p in range(chips):
            every[pl.ds(p * own_rows, own_rows), :] = g

    return vmem_call(body, "spread_gradient", plane.shape, (chips * own_rows, BLOCK))(plane, *shifted, limit)


def last_gradient(plane, shifted, limit, shards):
    def body(plane, one, two, three, limit, gradient, parts):
        g = gradient_of(plane, (one, two, three), limit)
        gradient[...] = g
        part = jnp.sum(jnp.sum(g * g, axis=0, keepdims=True), axis=1, keepdims=True)
        parts[...] = jnp.broadcast_to(part[None], parts.shape)

    return vmem_call(body, "last_gradient", plane.shape, (shards, 1, BLOCK))(plane, *shifted, limit)


def last_duals(duals, first, sumsq, second, parts, item_count):
    def body(duals, first, sumsq, second, parts, out):
        scale = jnp.sqrt(sumsq[0:1, :] / item_count + 1e-6)
        lam = jnp.maximum(duals[...] + 0.5 * first[...] / scale, 0.0)
        scale = jnp.sqrt(jnp.sum(parts[...], axis=0) / item_count + 1e-6)
        out[...] = jnp.maximum(lam + 0.5 * second[...] / scale, 0.0)

    return vmem_call(body, "last_duals", duals.shape)(duals, first, sumsq, second, parts)[0]


def local(candidates, affinity, exposure, lengths, item_limit, item_duals, *, grp_size, shard_size):
    chips = shard_size // 2
    same_core = [[2 * p + c for p in range(chips)] for c in range(2)]
    swap = [(g * shard_size + s, g * shard_size + (s ^ 1)) for g in range(grp_size) for s in range(shard_size)]
    members, slots = affinity.shape
    blocks = slots // BLOCK
    groups = members // SUB
    own_items = item_limit.shape[0]
    item_count = own_items * shard_size
    own_rows = own_items // BLOCK
    half = chips * own_rows
    full = 2 * half
    core = lax.axis_index("shard") % 2

    def swap_cores(x):
        return lax.ppermute(x, AXES, swap)

    def as_rows(x):
        return x.reshape(groups, SUB, blocks, BLOCK).transpose(0, 2, 1, 3).reshape(-1, BLOCK)

    def exchange(x):
        x = x.reshape(chips, 1, own_items)
        return lax.all_to_all(
            x, "shard", 0, 0, axis_index_groups=same_core, tiled=True).reshape(half, BLOCK)

    def gather_halves(every):
        every = exchange(every)
        return every, swap_cores(every)

    def reduce_loads(keep, send):
        chip = keep + swap_cores(send)
        plane = sum_chips(exchange(chip), chips)
        return plane, [
            lax.ppermute(plane, "grp", [(g, (g + d) % grp_size) for g in range(grp_size)])
            for d in range(1, grp_size)
        ]

    shard_of = candidates // own_rows
    gidx = (jnp.where(shard_of % 2 == core, 0, half) + (shard_of // 2) * own_rows + candidates % own_rows).reshape(-1)
    batch = gidx.reshape(-1, blocks)
    earlier = jnp.arange(blocks)[:, None] > jnp.arange(blocks)[None, :]
    copy = jnp.sum((batch[:, :, None] == batch[:, None, :]) & earlier, axis=2, dtype=jnp.int32)
    sidx = (batch + full * copy).reshape(groups, -1).T.reshape(-1)
    gidx = gidx.reshape(groups, -1).T.reshape(-1)
    ncopy = (jnp.max(copy) + 1).reshape(1)

    aff = as_rows(affinity)
    exp = as_rows(exposure)
    nlive = jnp.broadcast_to((lengths // BLOCK)[:, None], (members, BLOCK))
    limit = item_limit.reshape(own_rows, BLOCK)
    duals = item_duals.reshape(own_rows, BLOCK)

    own_d, other_d = gather_halves(spread_duals(duals, chips, core))
    keep, send = iteration_kernel(False, groups, blocks, half, item_count)(
        gidx, sidx, ncopy, own_d, other_d, aff, exp, nlive)
    first, every = spread_gradient(*reduce_loads(keep, send), limit, chips)

    own_g, other_g = gather_halves(every)
    keep, send, primal, sumsq = iteration_kernel(True, groups, blocks, half, item_count)(
        gidx, sidx, ncopy, own_d, other_d, own_g, other_g, aff, exp, nlive)
    second, parts = last_gradient(*reduce_loads(keep, send), limit, shard_size)
    parts = lax.all_to_all(parts, "shard", 0, 0, tiled=True)
    duals = last_duals(duals, first, sumsq, second, parts, item_count)

    primal = primal.reshape(groups, blocks, SUB, BLOCK).transpose(0, 2, 1, 3).reshape(members, slots)
    return primal, duals.reshape(-1)


def solution(mesh):
    placed = (
        P(("grp", "shard"), None),
        P(("grp", "shard"), None),
        P(("grp", "shard"), None),
        P(("grp", "shard")),
        P("shard"),
        P("shard"),
    )

    def run(*args):
        return local(*args, grp_size=mesh.shape["grp"], shard_size=mesh.shape["shard"])

    return jax.shard_map(
        run,
        mesh=mesh,
        in_specs=placed,
        out_specs=(P(("grp", "shard"), None), P("shard")),
        check_vma=False,
    )
```

```python
import jax
import jax.numpy as jnp
from jax import lax
from jax.experimental import pallas as pl
from jax.experimental.pallas import tpu as pltpu
from jax.sharding import PartitionSpec as P

BLOCK = 128
BISECT = 16
SUB = 8
COPIES = 8
DEAD = -1e30

AXES = ("grp", "shard")


def iteration_kernel(second, groups, blocks, half, item_count):
    full = 2 * half
    members = groups * SUB
    group_rows = SUB * blocks
    rows_all = groups * group_rows
    part = groups // 2
    quarter = part // 2
    part_rows = part * group_rows
    assert quarter * 4 == groups and part == BISECT and blocks % 2 == 0
    pieces = 4
    f32 = jnp.float32

    def body(*refs):
        if second:
            (gidx_in, sidx_in, ncopy, own_d, other_d, own_g, other_g, aff_in, exp_in, nlive,
             keep, send, primal_out, sumsq,
             table, work_a, work_b, acc_even, acc_odd, lo, up, peaks, sums, aff, exp, gidx, sidx, sem_in, sem_id,
             primal, sem_out) = refs
        else:
            (gidx_in, sidx_in, ncopy, own_d, other_d, aff_in, exp_in, nlive,
             keep, send,
             table, work_a, work_b, acc_even, acc_odd, lo, up, peaks, sums, aff, exp, gidx, sidx, sem_in, sem_id) = refs
        works = (work_a, work_b)
        accs = (acc_even, acc_odd)

        ids_in = [pltpu.make_async_copy(src, dst, sem_id.at[k])
                  for k, (src, dst) in enumerate(((gidx_in, gidx), (sidx_in, sidx)))]
        size = part_rows // pieces
        spans = [(k * size, size) for k in range(pieces)] + [(part_rows, part_rows)]
        loads = [[pltpu.make_async_copy(src.at[pl.ds(r, n), :], dst.at[pl.ds(r, n), :], sem_in.at[k, j])
                  for j, (src, dst) in enumerate(((aff_in, aff), (exp_in, exp)))]
                 for k, (r, n) in enumerate(spans)]
        ids_in[0].start()
        for pair in loads:
            for load in pair:
                load.start()
        ids_in[1].start()

        if second:
            def square(i, s):
                r = pl.multiple_of(i * SUB, SUB)
                a = own_g[pl.ds(r, SUB), :]
                b = other_g[pl.ds(r, SUB), :]
                return s + (a * a + b * b)

            s = lax.fori_loop(0, half // SUB, square, jnp.zeros((SUB, BLOCK), f32), unroll=8)
            total = jnp.sum(jnp.sum(s, axis=1, keepdims=True), axis=0, keepdims=True)
            total = jnp.broadcast_to(total, (SUB, BLOCK))
            sumsq[...] = total
            scale = jnp.sqrt(total / item_count + 1e-6)

            def fill_table(i, c):
                r = pl.multiple_of(i * SUB, SUB)
                for d, g, off in ((own_d, own_g, 0), (other_d, other_g, half)):
                    table[pl.ds(r + off, SUB), :] = jnp.maximum(
                        d[pl.ds(r, SUB), :] + 0.5 * g[pl.ds(r, SUB), :] / scale, 0.0)
                return c
        else:
            def fill_table(i, c):
                r = pl.multiple_of(i * SUB, SUB)
                table[pl.ds(r, SUB), :] = own_d[pl.ds(r, SUB), :]
                table[pl.ds(r + half, SUB), :] = other_d[pl.ds(r, SUB), :]
                return c

        lax.fori_loop(0, half // SUB, fill_table, 0, unroll=8)

        n = ncopy[0]
        fits = n <= COPIES
        used = jnp.where(fits, n, 1)
        zero = jnp.zeros((SUB, BLOCK), f32)
        dead = jnp.full((SUB, BLOCK), DEAD, f32)
        vregs = full // SUB
        per_step = vregs // (2 * BISECT)
        assert per_step * 2 * BISECT <= vregs and vregs % 16 == 0

        def clear(first, count):
            for acc in accs:
                some = acc.at[pl.ds(pl.multiple_of(first * SUB, SUB), count * SUB), :]
                for i in range(count):
                    some[pl.ds(i * SUB, SUB), :] = zero

        def clear_16(i, c):
            clear(16 * i, 16)
            return c

        lax.fori_loop(vregs // 16, used * vregs // 16, clear_16, 0)
        clear(per_step * 2 * BISECT, vregs - per_step * 2 * BISECT)

        def loop(first, last, f):
            def trip(i, c):
                f(i)
                return c

            lax.fori_loop(first, last, trip, 0)

        def picked(ids, j, g):
            return ids.at[pl.ds(j * groups, rows_all - j * groups)][g]

        def gather(h, g, first, count):
            rows = (h * part + g) * group_rows
            where = pl.multiple_of(rows + first * SUB, SUB)
            here = pl.multiple_of(g * group_rows + first * SUB, SUB)
            work = works[h].at[pl.ds(here, count * SUB), :]
            a_rows = aff.at[pl.ds(where, count * SUB), :]
            e_rows = exp.at[pl.ds(where, count * SUB), :]
            mrows = pl.ds(pl.multiple_of((h * part + g) * SUB, SUB), SUB)
            live = nlive[mrows, :] - first
            peak = peaks[mrows, :]
            for b in range(count):
                for s in range(SUB):
                    work[pl.ds(b * SUB + s, 1), :] = table[pl.ds(picked(gidx, s * blocks + b, h * part + g + first * groups), 1), :]
                now = pl.ds(b * SUB, SUB)
                v = (a_rows[now, :] - e_rows[now, :] * work[now, :]) * 2.0
                v = jnp.where(live > b, v, DEAD)
                work[now, :] = v
                peak = jnp.maximum(peak, v)
            peaks[mrows, :] = peak

        def start_bisection(h):
            for g in range(part):
                rows = pl.ds((h * part + g) * SUB, SUB)
                up[rows, :] = jnp.broadcast_to(jnp.max(peaks[rows, :], axis=1, keepdims=True), (SUB, BLOCK))
                lo[rows, :] = zero

        def fill_sums(h, q, *only):
            work = works[h].at[pl.ds(pl.multiple_of(q * (quarter * group_rows), SUB), quarter * group_rows), :]
            m0 = pl.multiple_of((h * part + q * quarter) * SUB, SUB)
            s0 = pl.multiple_of(q * (quarter * SUB), SUB)
            for g in only or range(quarter):
                rows = pl.ds(m0 + g * SUB, SUB)
                mid = (lo[rows, :] + up[rows, :]) * 0.5
                a = [None, None]
                for b in range(blocks):
                    v = jnp.clip(work[pl.ds(g * group_rows + b * SUB, SUB), :] - mid, 0.0, 1.0)
                    a[b % 2] = v if a[b % 2] is None else a[b % 2] + v
                sums[pl.ds(s0 + g * SUB, SUB), :] = a[0] + a[1]

        def lane_sums(q):
            s0 = pl.multiple_of(q * (quarter * SUB), SUB)
            return [jnp.sum(sums[pl.ds(s0 + g * SUB, SUB), :], axis=1, keepdims=True) for g in range(quarter)]

        def decide(h, q, fills):
            m0 = pl.multiple_of((h * part + q * quarter) * SUB, SUB)
            for g in range(quarter):
                rows = pl.ds(m0 + g * SUB, SUB)
                bigger = jnp.broadcast_to(fills[g], (SUB, BLOCK)) > 1.0
                low = lo[rows, :]
                high = up[rows, :]
                mid = (low + high) * 0.5
                lo[rows, :] = jnp.where(bigger, mid, low)
                up[rows, :] = jnp.where(bigger, high, mid)

        def bisect(h, beside):
            fill_sums(h, 0)

            def half_step(k):
                q = k % 2
                fills = lane_sums(q)
                steps = beside(k // 2, q)
                for g in range(quarter):
                    fill_sums(h, 1 - q, g)
                    for at, step in steps:
                        if at == g:
                            step()
                decide(h, q, fills)

            loop(0, 2 * BISECT, half_step)

        def allocate(h, g):
            rows = pl.multiple_of((h * part + g) * group_rows, SUB)
            here = pl.multiple_of(g * group_rows, SUB)
            mrows = pl.ds(pl.multiple_of((h * part + g) * SUB, SUB), SUB)
            th = up[mrows, :]
            live = nlive[mrows, :]
            for b in range(blocks):
                now = pl.ds(here + b * SUB, SUB)
                x = jnp.where(live > b, jnp.clip(works[h][now, :] - th, 0.0, 1.0), 0.0)
                if second:
                    primal[pl.ds(rows + b * SUB, SUB), :] = x
                works[h][now, :] = exp[pl.ds(rows + b * SUB, SUB), :] * x

        def scatter(h, g, first, count, parity=0):
            here = g * group_rows + first
            work = works[h]
            for s in range(count):
                where = [picked(sidx, s * blocks + b, h * part + g + first * blocks * groups) for b in range(blocks)]
                acc = accs[(s + parity) % 2]
                added = [acc[pl.ds(i, 1), :] + work[pl.ds(here + b * SUB + s, 1), :] for b, i in enumerate(where)]
                for i, v in zip(where, added):
                    acc[pl.ds(i, 1), :] = v

        for g in range(groups):
            peaks[pl.ds(g * SUB, SUB), :] = dead
        ids_in[0].wait()
        for k in range(pieces):
            for load in loads[k]:
                load.wait()
            loop(k * (part // pieces), (k + 1) * (part // pieces), lambda g: gather(0, g, 0, blocks))
        start_bisection(0)
        for load in loads[pieces]:
            load.wait()
        bisect(0, lambda g, q: [(quarter - 1, lambda: gather(1, g, q * (blocks // 2), blocks // 2)),
                                (quarter - 1, lambda: clear((2 * g + q) * per_step, per_step))])

        start_bisection(1)
        loop(0, part, lambda g: allocate(0, g))
        if second:
            stores = [pltpu.make_async_copy(
                primal.at[pl.ds(h * part_rows, part_rows), :],
                primal_out.at[pl.ds(h * part_rows, part_rows), :], sem_out.at[h]) for h in range(2)]
            stores[0].start()
        ids_in[1].wait()
        @pl.when(fits)
        def _():
            bisect(1, lambda g, q: [(2 * m, lambda m=m: scatter(0, g, q * (SUB // 2) + m, 1, m)) for m in range(SUB // 2)])

        @pl.when(jnp.logical_not(fits))
        def _():
            bisect(1, lambda g, q: [])

        loop(0, part, lambda g: allocate(1, g))
        if second:
            stores[1].start()

        @pl.when(fits)
        def _():
            loop(0, part, lambda g: scatter(1, g, 0, SUB))

        @pl.when(jnp.logical_not(fits))
        def _():
            def one(h, k):
                g = k // group_rows
                j = k - g * group_rows
                s = j // blocks
                i = gidx[j * groups + h * part + g]
                r = g * group_rows + (j - s * blocks) * SUB + s
                acc_even[pl.ds(i, 1), :] = acc_even[pl.ds(i, 1), :] + works[h][pl.ds(r, 1), :]

            for h in range(2):
                loop(0, part_rows, lambda k: one(h, k))

        def finish(i, c):
            r = pl.multiple_of(i * SUB, SUB)
            for out, o in ((keep, 0), (send, half)):
                out[pl.ds(r, SUB), :] = acc_even[pl.ds(r + o, SUB), :] + acc_odd[pl.ds(r + o, SUB), :]
            return c

        lax.fori_loop(0, half // SUB, finish, 0, unroll=8)

        def finish_copy(t, c):
            def more(i, c):
                r = pl.multiple_of(i * SUB, SUB)
                a = pl.multiple_of(t * full + r, SUB)
                for out, o in ((keep, 0), (send, half)):
                    out[pl.ds(r, SUB), :] += acc_even[pl.ds(a + o, SUB), :] + acc_odd[pl.ds(a + o, SUB), :]
                return c

            return lax.fori_loop(0, half // SUB, more, c, unroll=8)

        lax.fori_loop(1, used, finish_copy, 0)
        if second:
            for store in stores:
                store.wait()

    smem = pl.BlockSpec(memory_space=pltpu.SMEM)
    vmem = pl.BlockSpec(memory_space=pltpu.VMEM)
    left = pl.BlockSpec(memory_space=pltpu.HBM)
    outs = [jax.ShapeDtypeStruct((half, BLOCK), f32)] * 2
    out_specs = [vmem] * 2
    scratch = [
        pltpu.VMEM((full, BLOCK), f32),
        pltpu.VMEM((part_rows, BLOCK), f32),
        pltpu.VMEM((part_rows, BLOCK), f32),
        pltpu.VMEM((COPIES * full, BLOCK), f32),
        pltpu.VMEM((COPIES * full, BLOCK), f32),
        pltpu.VMEM((members, BLOCK), f32),
        pltpu.VMEM((members, BLOCK), f32),
        pltpu.VMEM((members, BLOCK), f32),
        pltpu.VMEM((part * SUB, BLOCK), f32),
        pltpu.VMEM((rows_all, BLOCK), f32),
        pltpu.VMEM((rows_all, BLOCK), f32),
        pltpu.SMEM((rows_all,), jnp.int32),
        pltpu.SMEM((rows_all,), jnp.int32),
        pltpu.SemaphoreType.DMA((pieces + 1, 2)),
        pltpu.SemaphoreType.DMA((2,)),
    ]
    if second:
        outs += [jax.ShapeDtypeStruct((rows_all, BLOCK), f32), jax.ShapeDtypeStruct((SUB, BLOCK), f32)]
        out_specs += [left, vmem]
        scratch += [pltpu.VMEM((rows_all, BLOCK), f32), pltpu.SemaphoreType.DMA((2,))]
    tables = [vmem] * (4 if second else 2)
    call = pl.pallas_call(
        body,
        out_shape=outs,
        in_specs=[left, left, smem] + tables + [left, left, vmem],
        out_specs=out_specs,
        scratch_shapes=scratch,
        compiler_params=pltpu.CompilerParams(vmem_limit_bytes=48 << 20),
        name="iterate2" if second else "iterate1",
    )

    def run(gidx, sidx, ncopy, *rest):
        *tables, aff, exp, nlive = rest
        aff, exp = (pltpu.with_memory_space_constraint(x, pltpu.HBM) for x in (aff, exp))
        return call(gidx, sidx, ncopy, *tables, aff, exp, nlive)

    return run


def vmem_call(body, name, *outs):
    spec = pl.BlockSpec(memory_space=pltpu.VMEM)
    return pl.pallas_call(
        body,
        out_shape=[jax.ShapeDtypeStruct(shape, jnp.float32) for shape in outs],
        out_specs=[spec] * len(outs),
        compiler_params=pltpu.CompilerParams(vmem_limit_bytes=4 << 20),
        name=name,
    )


def spread_duals(x, chips, core):
    own_rows = x.shape[0]

    def body(x, core, every):
        for p in range(chips):
            every[pl.ds(p * own_rows, own_rows), :] = x[...]

    return vmem_call(body, "spread_duals", (chips * own_rows, BLOCK))(
        x, jnp.full((SUB, BLOCK), core, jnp.int32))[0]


def sum_chips(x, chips):
    own_rows = x.shape[0] // chips

    def body(x, out):
        parts = [x[pl.ds(p * own_rows, own_rows), :] for p in range(chips)]
        while len(parts) > 1:
            parts = [a + b for a, b in zip(parts[::2], parts[1::2])]
        out[...] = parts[0]

    return vmem_call(body, "sum_chips", (own_rows, BLOCK))(x)[0]


def gradient_of(plane, shifted, limit):
    one, two, three = shifted
    return ((plane[...] + two[...]) + (one[...] + three[...])) - limit[...]


def spread_gradient(plane, shifted, limit, chips):
    own_rows = plane.shape[0]

    def body(plane, one, two, three, limit, gradient, every):
        g = gradient_of(plane, (one, two, three), limit)
        gradient[...] = g
        for p in range(chips):
            every[pl.ds(p * own_rows, own_rows), :] = g

    return vmem_call(body, "spread_gradient", plane.shape, (chips * own_rows, BLOCK))(plane, *shifted, limit)


def last_gradient(plane, shifted, limit, shards):
    def body(plane, one, two, three, limit, gradient, parts):
        g = gradient_of(plane, (one, two, three), limit)
        gradient[...] = g
        part = jnp.sum(jnp.sum(g * g, axis=0, keepdims=True), axis=1, keepdims=True)
        parts[...] = jnp.broadcast_to(part[None], parts.shape)

    return vmem_call(body, "last_gradient", plane.shape, (shards, 1, BLOCK))(plane, *shifted, limit)


def last_duals(duals, first, sumsq, second, parts, item_count):
    def body(duals, first, sumsq, second, parts, out):
        scale = jnp.sqrt(sumsq[0:1, :] / item_count + 1e-6)
        lam = jnp.maximum(duals[...] + 0.5 * first[...] / scale, 0.0)
        scale = jnp.sqrt(jnp.sum(parts[...], axis=0) / item_count + 1e-6)
        out[...] = jnp.maximum(lam + 0.5 * second[...] / scale, 0.0)

    return vmem_call(body, "last_duals", duals.shape)(duals, first, sumsq, second, parts)[0]


def local(candidates, affinity, exposure, lengths, item_limit, item_duals, *, grp_size, shard_size):
    chips = shard_size // 2
    same_core = [[2 * p + c for p in range(chips)] for c in range(2)]
    swap = [(g * shard_size + s, g * shard_size + (s ^ 1)) for g in range(grp_size) for s in range(shard_size)]
    members, slots = affinity.shape
    blocks = slots // BLOCK
    groups = members // SUB
    own_items = item_limit.shape[0]
    item_count = own_items * shard_size
    own_rows = own_items // BLOCK
    half = chips * own_rows
    full = 2 * half
    core = lax.axis_index("shard") % 2

    def swap_cores(x):
        return lax.ppermute(x, AXES, swap)

    def as_rows(x):
        return x.reshape(groups, SUB, blocks, BLOCK).transpose(0, 2, 1, 3).reshape(-1, BLOCK)

    def exchange(x):
        x = x.reshape(chips, 1, own_items)
        return lax.all_to_all(
            x, "shard", 0, 0, axis_index_groups=same_core, tiled=True).reshape(half, BLOCK)

    def gather_halves(every):
        every = exchange(every)
        return every, swap_cores(every)

    def reduce_loads(keep, send):
        chip = keep + swap_cores(send)
        plane = sum_chips(exchange(chip), chips)
        return plane, [
            lax.ppermute(plane, "grp", [(g, (g + d) % grp_size) for g in range(grp_size)])
            for d in range(1, grp_size)
        ]

    shard_of = candidates // own_rows
    gidx = (jnp.where(shard_of % 2 == core, 0, half) + (shard_of // 2) * own_rows + candidates % own_rows).reshape(-1)
    batch = gidx.reshape(-1, blocks)
    earlier = jnp.arange(blocks)[:, None] > jnp.arange(blocks)[None, :]
    copy = jnp.sum((batch[:, :, None] == batch[:, None, :]) & earlier, axis=2, dtype=jnp.int32)
    sidx = (batch + full * copy).reshape(groups, -1).T.reshape(-1)
    gidx = gidx.reshape(groups, -1).T.reshape(-1)
    ncopy = (jnp.max(copy) + 1).reshape(1)

    aff = as_rows(affinity)
    exp = as_rows(exposure)
    nlive = jnp.broadcast_to((lengths // BLOCK)[:, None], (members, BLOCK))
    limit = item_limit.reshape(own_rows, BLOCK)
    duals = item_duals.reshape(own_rows, BLOCK)

    own_d, other_d = gather_halves(spread_duals(duals, chips, core))
    keep, send = iteration_kernel(False, groups, blocks, half, item_count)(
        gidx, sidx, ncopy, own_d, other_d, aff, exp, nlive)
    first, every = spread_gradient(*reduce_loads(keep, send), limit, chips)

    own_g, other_g = gather_halves(every)
    keep, send, primal, sumsq = iteration_kernel(True, groups, blocks, half, item_count)(
        gidx, sidx, ncopy, own_d, other_d, own_g, other_g, aff, exp, nlive)
    second, parts = last_gradient(*reduce_loads(keep, send), limit, shard_size)
    parts = lax.all_to_all(parts, "shard", 0, 0, tiled=True)
    duals = last_duals(duals, first, sumsq, second, parts, item_count)

    primal = primal.reshape(groups, blocks, SUB, BLOCK).transpose(0, 2, 1, 3).reshape(members, slots)
    return primal, duals.reshape(-1)


def solution(mesh):
    placed = (
        P(("grp", "shard"), None),
        P(("grp", "shard"), None),
        P(("grp", "shard"), None),
        P(("grp", "shard")),
        P("shard"),
        P("shard"),
    )

    def run(*args):
        return local(*args, grp_size=mesh.shape["grp"], shard_size=mesh.shape["shard"])

    return jax.shard_map(
        run,
        mesh=mesh,
        in_specs=placed,
        out_specs=(P(("grp", "shard"), None), P("shard")),
        check_vma=False,
    )
```

```python
import jax
import jax.numpy as jnp
from jax import lax
from jax.experimental import pallas as pl
from jax.experimental.pallas import tpu as pltpu
from jax.sharding import PartitionSpec as P

BLOCK = 128
BISECT = 16
SUB = 8
COPIES = 8
DEAD = -1e30

AXES = ("grp", "shard")


def iteration_kernel(second, groups, blocks, half, item_count):
    full = 2 * half
    members = groups * SUB
    group_rows = SUB * blocks
    rows_all = groups * group_rows
    part = groups // 2
    quarter = part // 2
    part_rows = part * group_rows
    assert quarter * 4 == groups and part == BISECT and blocks % 2 == 0
    pieces = 4
    f32 = jnp.float32

    def body(*refs):
        if second:
            (gidx_in, sidx_in, ncopy, own_d, other_d, own_g, other_g, aff_in, exp_in, nlive,
             keep, send, primal_out, sumsq,
             table, work_a, work_b, acc_even, acc_odd, lo, up, peaks, sums, aff, exp, gidx, sidx, sem_in, sem_id,
             primal, sem_out) = refs
        else:
            (gidx_in, sidx_in, ncopy, own_d, other_d, aff_in, exp_in, nlive,
             keep, send,
             table, work_a, work_b, acc_even, acc_odd, lo, up, peaks, sums, aff, exp, gidx, sidx, sem_in, sem_id) = refs
        works = (work_a, work_b)
        accs = (acc_even, acc_odd)

        ids_in = [pltpu.make_async_copy(src, dst, sem_id.at[k])
                  for k, (src, dst) in enumerate(((gidx_in, gidx), (sidx_in, sidx)))]
        size = part_rows // pieces
        spans = [(k * size, size) for k in range(pieces)] + [(part_rows, part_rows)]
        loads = [[pltpu.make_async_copy(src.at[pl.ds(r, n), :], dst.at[pl.ds(r, n), :], sem_in.at[k, j])
                  for j, (src, dst) in enumerate(((aff_in, aff), (exp_in, exp)))]
                 for k, (r, n) in enumerate(spans)]
        ids_in[0].start()
        for pair in loads:
            for load in pair:
                load.start()
        ids_in[1].start()

        if second:
            def square(i, s):
                r = pl.multiple_of(i * SUB, SUB)
                a = own_g[pl.ds(r, SUB), :]
                b = other_g[pl.ds(r, SUB), :]
                return s + (a * a + b * b)

            s = lax.fori_loop(0, half // SUB, square, jnp.zeros((SUB, BLOCK), f32), unroll=8)
            total = jnp.sum(jnp.sum(s, axis=1, keepdims=True), axis=0, keepdims=True)
            total = jnp.broadcast_to(total, (SUB, BLOCK))
            sumsq[...] = total
            scale = jnp.sqrt(total / item_count + 1e-6)

            def fill_table(i, c):
                r = pl.multiple_of(i * SUB, SUB)
                for d, g, off in ((own_d, own_g, 0), (other_d, other_g, half)):
                    table[pl.ds(r + off, SUB), :] = jnp.maximum(
                        d[pl.ds(r, SUB), :] + 0.5 * g[pl.ds(r, SUB), :] / scale, 0.0)
                return c
        else:
            def fill_table(i, c):
                r = pl.multiple_of(i * SUB, SUB)
                table[pl.ds(r, SUB), :] = own_d[pl.ds(r, SUB), :]
                table[pl.ds(r + half, SUB), :] = other_d[pl.ds(r, SUB), :]
                return c

        lax.fori_loop(0, half // SUB, fill_table, 0, unroll=8)

        n = ncopy[0]
        fits = n <= COPIES
        used = jnp.where(fits, jnp.maximum(n, 2), 2)
        zero = jnp.zeros((SUB, BLOCK), f32)
        dead = jnp.full((SUB, BLOCK), DEAD, f32)
        vregs = full // SUB
        per_step = vregs // (2 * BISECT)
        assert per_step * 2 * BISECT <= vregs and vregs % 16 == 0

        def clear(first, count):
            for acc in accs:
                some = acc.at[pl.ds(pl.multiple_of(first * SUB, SUB), count * SUB), :]
                for i in range(count):
                    some[pl.ds(i * SUB, SUB), :] = zero

        def clear_16(i, c):
            clear(16 * i, 16)
            return c

        lax.fori_loop(vregs // 16, used * vregs // 16, clear_16, 0)
        clear(per_step * 2 * BISECT, vregs - per_step * 2 * BISECT)

        def loop(first, last, f):
            def trip(i, c):
                f(i)
                return c

            lax.fori_loop(first, last, trip, 0)

        def picked(ids, j, g):
            return ids.at[pl.ds(j * groups, rows_all - j * groups)][g]

        def gather(h, g, first, count):
            rows = (h * part + g) * group_rows
            where = pl.multiple_of(rows + first * SUB, SUB)
            here = pl.multiple_of(g * group_rows + first * SUB, SUB)
            work = works[h].at[pl.ds(here, count * SUB), :]
            a_rows = aff.at[pl.ds(where, count * SUB), :]
            e_rows = exp.at[pl.ds(where, count * SUB), :]
            mrows = pl.ds(pl.multiple_of((h * part + g) * SUB, SUB), SUB)
            live = nlive[mrows, :] - first
            peak = peaks[mrows, :]
            for b in range(count):
                for s in range(SUB):
                    work[pl.ds(b * SUB + s, 1), :] = table[pl.ds(picked(gidx, s * blocks + b, h * part + g + first * groups), 1), :]
                now = pl.ds(b * SUB, SUB)
                v = (a_rows[now, :] - e_rows[now, :] * work[now, :]) * 2.0
                v = jnp.where(live > b, v, DEAD)
                work[now, :] = v
                peak = jnp.maximum(peak, v)
            peaks[mrows, :] = peak

        def start_bisection(h):
            for g in range(part):
                rows = pl.ds((h * part + g) * SUB, SUB)
                up[rows, :] = jnp.broadcast_to(jnp.max(peaks[rows, :], axis=1, keepdims=True), (SUB, BLOCK))
                lo[rows, :] = zero

        def fill_sums(h, q, *only):
            work = works[h].at[pl.ds(pl.multiple_of(q * (quarter * group_rows), SUB), quarter * group_rows), :]
            m0 = pl.multiple_of((h * part + q * quarter) * SUB, SUB)
            s0 = pl.multiple_of(q * (quarter * SUB), SUB)
            for g in only or range(quarter):
                rows = pl.ds(m0 + g * SUB, SUB)
                mid = (lo[rows, :] + up[rows, :]) * 0.5
                a = [None, None]
                for b in range(blocks):
                    v = jnp.clip(work[pl.ds(g * group_rows + b * SUB, SUB), :] - mid, 0.0, 1.0)
                    a[b % 2] = v if a[b % 2] is None else a[b % 2] + v
                sums[pl.ds(s0 + g * SUB, SUB), :] = a[0] + a[1]

        def lane_sums(q):
            s0 = pl.multiple_of(q * (quarter * SUB), SUB)
            return [jnp.sum(sums[pl.ds(s0 + g * SUB, SUB), :], axis=1, keepdims=True) for g in range(quarter)]

        def decide(h, q, fills):
            m0 = pl.multiple_of((h * part + q * quarter) * SUB, SUB)
            for g in range(quarter):
                rows = pl.ds(m0 + g * SUB, SUB)
                bigger = jnp.broadcast_to(fills[g], (SUB, BLOCK)) > 1.0
                low = lo[rows, :]
                high = up[rows, :]
                mid = (low + high) * 0.5
                lo[rows, :] = jnp.where(bigger, mid, low)
                up[rows, :] = jnp.where(bigger, high, mid)

        def bisect(h, beside):
            fill_sums(h, 0)

            def half_step(k):
                q = k % 2
                fills = lane_sums(q)
                steps = beside(k // 2, q)
                for g in range(quarter):
                    fill_sums(h, 1 - q, g)
                    for at, step in steps:
                        if at == g:
                            step()
                decide(h, q, fills)

            loop(0, 2 * BISECT, half_step)

        def allocate(h, g):
            rows = pl.multiple_of((h * part + g) * group_rows, SUB)
            here = pl.multiple_of(g * group_rows, SUB)
            mrows = pl.ds(pl.multiple_of((h * part + g) * SUB, SUB), SUB)
            th = up[mrows, :]
            live = nlive[mrows, :]
            for b in range(blocks):
                now = pl.ds(here + b * SUB, SUB)
                x = jnp.where(live > b, jnp.clip(works[h][now, :] - th, 0.0, 1.0), 0.0)
                if second:
                    primal[pl.ds(rows + b * SUB, SUB), :] = x
                works[h][now, :] = exp[pl.ds(rows + b * SUB, SUB), :] * x

        def scatter(h, g, first, count, parity=0):
            here = g * group_rows + first
            work = works[h]
            for s in range(count):
                where = [picked(sidx, s * blocks + b, h * part + g + first * blocks * groups) for b in range(blocks)]
                acc = accs[(s + parity) % 2]
                added = [acc[pl.ds(i, 1), :] + work[pl.ds(here + b * SUB + s, 1), :] for b, i in enumerate(where)]
                for i, v in zip(where, added):
                    acc[pl.ds(i, 1), :] = v

        for g in range(groups):
            peaks[pl.ds(g * SUB, SUB), :] = dead
        ids_in[0].wait()
        for k in range(pieces):
            for load in loads[k]:
                load.wait()
            loop(k * (part // pieces), (k + 1) * (part // pieces), lambda g: gather(0, g, 0, blocks))
        start_bisection(0)
        for load in loads[pieces]:
            load.wait()
        bisect(0, lambda g, q: [(quarter - 1, lambda: gather(1, g, q * (blocks // 2), blocks // 2)),
                                (quarter - 1, lambda: clear((2 * g + q) * per_step, per_step))])

        start_bisection(1)
        loop(0, part, lambda g: allocate(0, g))
        if second:
            stores = [pltpu.make_async_copy(
                primal.at[pl.ds(h * part_rows, part_rows), :],
                primal_out.at[pl.ds(h * part_rows, part_rows), :], sem_out.at[h]) for h in range(2)]
            stores[0].start()
        ids_in[1].wait()
        @pl.when(fits)
        def _():
            bisect(1, lambda g, q: [(2 * m, lambda m=m: scatter(0, g, q * (SUB // 2) + m, 1, m)) for m in range(SUB // 2)])

        @pl.when(jnp.logical_not(fits))
        def _():
            bisect(1, lambda g, q: [])

        loop(0, part, lambda g: allocate(1, g))
        if second:
            stores[1].start()

        @pl.when(fits)
        def _():
            loop(0, part, lambda g: scatter(1, g, 0, SUB))

        @pl.when(jnp.logical_not(fits))
        def _():
            def one(h, k):
                g = k // group_rows
                j = k - g * group_rows
                s = j // blocks
                i = gidx[j * groups + h * part + g]
                r = g * group_rows + (j - s * blocks) * SUB + s
                acc_even[pl.ds(i, 1), :] = acc_even[pl.ds(i, 1), :] + works[h][pl.ds(r, 1), :]

            for h in range(2):
                loop(0, part_rows, lambda k: one(h, k))

        def finish(i, c):
            r = pl.multiple_of(i * SUB, SUB)
            for out, o in ((keep, 0), (send, half)):
                out[pl.ds(r, SUB), :] = (
                    (acc_even[pl.ds(r + o, SUB), :] + acc_odd[pl.ds(r + o, SUB), :])
                    + (acc_even[pl.ds(r + (full + o), SUB), :] + acc_odd[pl.ds(r + (full + o), SUB), :]))
            return c

        lax.fori_loop(0, half // SUB, finish, 0, unroll=8)

        def finish_copy(t, c):
            def more(i, c):
                r = pl.multiple_of(i * SUB, SUB)
                a = pl.multiple_of(t * full + r, SUB)
                for out, o in ((keep, 0), (send, half)):
                    out[pl.ds(r, SUB), :] += acc_even[pl.ds(a + o, SUB), :] + acc_odd[pl.ds(a + o, SUB), :]
                return c

            return lax.fori_loop(0, half // SUB, more, c, unroll=8)

        lax.fori_loop(2, used, finish_copy, 0)
        if second:
            for store in stores:
                store.wait()

    smem = pl.BlockSpec(memory_space=pltpu.SMEM)
    vmem = pl.BlockSpec(memory_space=pltpu.VMEM)
    left = pl.BlockSpec(memory_space=pltpu.HBM)
    outs = [jax.ShapeDtypeStruct((half, BLOCK), f32)] * 2
    out_specs = [vmem] * 2
    scratch = [
        pltpu.VMEM((full, BLOCK), f32),
        pltpu.VMEM((part_rows, BLOCK), f32),
        pltpu.VMEM((part_rows, BLOCK), f32),
        pltpu.VMEM((COPIES * full, BLOCK), f32),
        pltpu.VMEM((COPIES * full, BLOCK), f32),
        pltpu.VMEM((members, BLOCK), f32),
        pltpu.VMEM((members, BLOCK), f32),
        pltpu.VMEM((members, BLOCK), f32),
        pltpu.VMEM((part * SUB, BLOCK), f32),
        pltpu.VMEM((rows_all, BLOCK), f32),
        pltpu.VMEM((rows_all, BLOCK), f32),
        pltpu.SMEM((rows_all,), jnp.int32),
        pltpu.SMEM((rows_all,), jnp.int32),
        pltpu.SemaphoreType.DMA((pieces + 1, 2)),
        pltpu.SemaphoreType.DMA((2,)),
    ]
    if second:
        outs += [jax.ShapeDtypeStruct((rows_all, BLOCK), f32), jax.ShapeDtypeStruct((SUB, BLOCK), f32)]
        out_specs += [left, vmem]
        scratch += [pltpu.VMEM((rows_all, BLOCK), f32), pltpu.SemaphoreType.DMA((2,))]
    tables = [vmem] * (4 if second else 2)
    call = pl.pallas_call(
        body,
        out_shape=outs,
        in_specs=[left, left, smem] + tables + [left, left, vmem],
        out_specs=out_specs,
        scratch_shapes=scratch,
        compiler_params=pltpu.CompilerParams(vmem_limit_bytes=48 << 20),
        name="iterate2" if second else "iterate1",
    )

    def run(gidx, sidx, ncopy, *rest):
        *tables, aff, exp, nlive = rest
        aff, exp = (pltpu.with_memory_space_constraint(x, pltpu.HBM) for x in (aff, exp))
        return call(gidx, sidx, ncopy, *tables, aff, exp, nlive)

    return run


def vmem_call(body, name, *outs):
    spec = pl.BlockSpec(memory_space=pltpu.VMEM)
    return pl.pallas_call(
        body,
        out_shape=[jax.ShapeDtypeStruct(shape, jnp.float32) for shape in outs],
        out_specs=[spec] * len(outs),
        compiler_params=pltpu.CompilerParams(vmem_limit_bytes=4 << 20),
        name=name,
    )


def spread_duals(x, chips, core):
    own_rows = x.shape[0]

    def body(x, core, every):
        for p in range(chips):
            every[pl.ds(p * own_rows, own_rows), :] = x[...]

    return vmem_call(body, "spread_duals", (chips * own_rows, BLOCK))(
        x, jnp.full((SUB, BLOCK), core, jnp.int32))[0]


def sum_chips(x, chips):
    own_rows = x.shape[0] // chips

    def body(x, out):
        parts = [x[pl.ds(p * own_rows, own_rows), :] for p in range(chips)]
        while len(parts) > 1:
            parts = [a + b for a, b in zip(parts[::2], parts[1::2])]
        out[...] = parts[0]

    return vmem_call(body, "sum_chips", (own_rows, BLOCK))(x)[0]


def gradient_of(plane, shifted, limit):
    one, three, two = shifted
    return ((plane[...] + two[...]) + (one[...] + three[...])) - limit[...]


def spread_gradient(plane, shifted, limit, chips):
    own_rows = plane.shape[0]

    def body(plane, one, three, two, limit, gradient, every):
        g = gradient_of(plane, (one, three, two), limit)
        gradient[...] = g
        for p in range(chips):
            every[pl.ds(p * own_rows, own_rows), :] = g

    return vmem_call(body, "spread_gradient", plane.shape, (chips * own_rows, BLOCK))(plane, *shifted, limit)


def last_gradient(plane, shifted, limit, shards):
    def body(plane, one, three, two, limit, gradient, parts):
        g = gradient_of(plane, (one, three, two), limit)
        gradient[...] = g
        part = jnp.sum(jnp.sum(g * g, axis=0, keepdims=True), axis=1, keepdims=True)
        parts[...] = jnp.broadcast_to(part[None], parts.shape)

    return vmem_call(body, "last_gradient", plane.shape, (shards, 1, BLOCK))(plane, *shifted, limit)


def last_duals(duals, first, sumsq, second, parts, item_count):
    def body(duals, first, sumsq, second, parts, out):
        scale = jnp.sqrt(sumsq[0:1, :] / item_count + 1e-6)
        lam = jnp.maximum(duals[...] + 0.5 * first[...] / scale, 0.0)
        scale = jnp.sqrt(jnp.sum(parts[...], axis=0) / item_count + 1e-6)
        out[...] = jnp.maximum(lam + 0.5 * second[...] / scale, 0.0)

    return vmem_call(body, "last_duals", duals.shape)(duals, first, sumsq, second, parts)[0]


def local(candidates, affinity, exposure, lengths, item_limit, item_duals, *, grp_size, shard_size):
    chips = shard_size // 2
    same_core = [[2 * p + c for p in range(chips)] for c in range(2)]
    swap = [(g * shard_size + s, g * shard_size + (s ^ 1)) for g in range(grp_size) for s in range(shard_size)]
    members, slots = affinity.shape
    blocks = slots // BLOCK
    groups = members // SUB
    own_items = item_limit.shape[0]
    item_count = own_items * shard_size
    own_rows = own_items // BLOCK
    half = chips * own_rows
    full = 2 * half
    core = lax.axis_index("shard") % 2

    def swap_cores(x):
        return lax.ppermute(x, AXES, swap)

    def as_rows(x):
        return x.reshape(groups, SUB, blocks, BLOCK).transpose(0, 2, 1, 3).reshape(-1, BLOCK)

    def exchange(x):
        x = x.reshape(chips, 1, own_items)
        return lax.all_to_all(
            x, "shard", 0, 0, axis_index_groups=same_core, tiled=True).reshape(half, BLOCK)

    def gather_halves(every):
        every = exchange(every)
        return every, swap_cores(every)

    def reduce_loads(keep, send):
        chip = keep + swap_cores(send)
        plane = sum_chips(exchange(chip), chips)
        return plane, [
            lax.ppermute(plane, "grp", [(g, (g + d) % grp_size) for g in range(grp_size)])
            for d in (1, 3, 2)
        ]

    shard_of = candidates // own_rows
    gidx = (jnp.where(shard_of % 2 == core, 0, half) + (shard_of // 2) * own_rows + candidates % own_rows).reshape(-1)
    batch = gidx.reshape(-1, blocks)
    earlier = jnp.arange(blocks)[:, None] > jnp.arange(blocks)[None, :]
    copy = jnp.sum((batch[:, :, None] == batch[:, None, :]) & earlier, axis=2, dtype=jnp.int32)
    sidx = (batch + full * copy).reshape(groups, -1).T.reshape(-1)
    gidx = gidx.reshape(groups, -1).T.reshape(-1)
    ncopy = (jnp.max(copy) + 1).reshape(1)

    aff = as_rows(affinity)
    exp = as_rows(exposure)
    nlive = jnp.broadcast_to((lengths // BLOCK)[:, None], (members, BLOCK))
    limit = item_limit.reshape(own_rows, BLOCK)
    duals = item_duals.reshape(own_rows, BLOCK)

    own_d, other_d = gather_halves(spread_duals(duals, chips, core))
    keep, send = iteration_kernel(False, groups, blocks, half, item_count)(
        gidx, sidx, ncopy, own_d, other_d, aff, exp, nlive)
    first, every = spread_gradient(*reduce_loads(keep, send), limit, chips)

    own_g, other_g = gather_halves(every)
    keep, send, primal, sumsq = iteration_kernel(True, groups, blocks, half, item_count)(
        gidx, sidx, ncopy, own_d, other_d, own_g, other_g, aff, exp, nlive)
    second, parts = last_gradient(*reduce_loads(keep, send), limit, shard_size)
    parts = lax.all_to_all(parts, "shard", 0, 0, tiled=True)
    duals = last_duals(duals, first, sumsq, second, parts, item_count)

    primal = primal.reshape(groups, blocks, SUB, BLOCK).transpose(0, 2, 1, 3).reshape(members, slots)
    return primal, duals.reshape(-1)


def solution(mesh):
    placed = (
        P(("grp", "shard"), None),
        P(("grp", "shard"), None),
        P(("grp", "shard"), None),
        P(("grp", "shard")),
        P("shard"),
        P("shard"),
    )

    def run(*args):
        return local(*args, grp_size=mesh.shape["grp"], shard_size=mesh.shape["shard"])

    return jax.shard_map(
        run,
        mesh=mesh,
        in_specs=placed,
        out_specs=(P(("grp", "shard"), None), P("shard")),
        check_vma=False,
    )
```

```python
import jax
import jax.numpy as jnp
from jax import lax
from jax.experimental import pallas as pl
from jax.experimental.pallas import tpu as pltpu
from jax.sharding import PartitionSpec as P

BLOCK = 128
BISECT = 16
SUB = 8
COPIES = 8
DEAD = -1e30

AXES = ("grp", "shard")


def iteration_kernel(second, groups, blocks, half, item_count):
    full = 2 * half
    members = groups * SUB
    group_rows = SUB * blocks
    rows_all = groups * group_rows
    part = groups // 2
    quarter = part // 2
    part_rows = part * group_rows
    assert quarter * 4 == groups and part == BISECT and blocks % 2 == 0
    pieces = 4
    f32 = jnp.float32

    def body(*refs):
        if second:
            (gidx_in, sidx_in, ncopy, own_d, other_d, own_g, other_g, aff_in, exp_in, nlive,
             keep, send, primal_out, sumsq,
             table, work_a, work_b, acc_even, acc_odd, lo, up, peaks, sums, aff, exp, gidx, sidx, sem_in, sem_id,
             primal, sem_out) = refs
        else:
            (gidx_in, sidx_in, ncopy, own_d, other_d, aff_in, exp_in, nlive,
             keep, send,
             table, work_a, work_b, acc_even, acc_odd, lo, up, peaks, sums, aff, exp, gidx, sidx, sem_in, sem_id) = refs
        works = (work_a, work_b)
        accs = (acc_even, acc_odd)

        ids_in = [pltpu.make_async_copy(src, dst, sem_id.at[k])
                  for k, (src, dst) in enumerate(((gidx_in, gidx), (sidx_in, sidx)))]
        size = part_rows // pieces
        spans = [(k * size, size) for k in range(pieces)] + [(part_rows, part_rows)]
        loads = [[pltpu.make_async_copy(src.at[pl.ds(r, n), :], dst.at[pl.ds(r, n), :], sem_in.at[k, j])
                  for j, (src, dst) in enumerate(((aff_in, aff), (exp_in, exp)))]
                 for k, (r, n) in enumerate(spans)]
        ids_in[0].start()
        for pair in loads:
            for load in pair:
                load.start()
        ids_in[1].start()

        if second:
            def square(i, s):
                r = pl.multiple_of(i * SUB, SUB)
                a = own_g[pl.ds(r, SUB), :]
                b = other_g[pl.ds(r, SUB), :]
                return s + (a * a + b * b)

            s = lax.fori_loop(0, half // SUB, square, jnp.zeros((SUB, BLOCK), f32), unroll=8)
            total = jnp.sum(jnp.sum(s, axis=1, keepdims=True), axis=0, keepdims=True)
            total = jnp.broadcast_to(total, (SUB, BLOCK))
            sumsq[...] = total
            scale = jnp.sqrt(total / item_count + 1e-6)

            def fill_table(i, c):
                r = pl.multiple_of(i * SUB, SUB)
                for d, g, off in ((own_d, own_g, 0), (other_d, other_g, half)):
                    table[pl.ds(r + off, SUB), :] = jnp.maximum(
                        d[pl.ds(r, SUB), :] + 0.5 * g[pl.ds(r, SUB), :] / scale, 0.0)
                return c
        else:
            def fill_table(i, c):
                r = pl.multiple_of(i * SUB, SUB)
                table[pl.ds(r, SUB), :] = own_d[pl.ds(r, SUB), :]
                table[pl.ds(r + half, SUB), :] = other_d[pl.ds(r, SUB), :]
                return c

        lax.fori_loop(0, half // SUB, fill_table, 0, unroll=8)

        n = ncopy[0]
        fits = n <= COPIES
        used = jnp.where(fits, jnp.maximum(n, 2), 2)
        zero = jnp.zeros((SUB, BLOCK), f32)
        dead = jnp.full((SUB, BLOCK), DEAD, f32)
        vregs = full // SUB
        per_step = vregs // (2 * BISECT)
        assert per_step * 2 * BISECT <= vregs and vregs % 16 == 0

        def clear(first, count):
            for acc in accs:
                some = acc.at[pl.ds(pl.multiple_of(first * SUB, SUB), count * SUB), :]
                for i in range(count):
                    some[pl.ds(i * SUB, SUB), :] = zero

        def clear_16(i, c):
            clear(16 * i, 16)
            return c

        lax.fori_loop(vregs // 16, used * vregs // 16, clear_16, 0)
        clear(per_step * 2 * BISECT, vregs - per_step * 2 * BISECT)

        def loop(first, last, f):
            def trip(i, c):
                f(i)
                return c

            lax.fori_loop(first, last, trip, 0)

        def picked(ids, j, g):
            return ids.at[pl.ds(j * groups, rows_all - j * groups)][g]

        def gather(h, g, first, count):
            rows = (h * part + g) * group_rows
            where = pl.multiple_of(rows + first * SUB, SUB)
            here = pl.multiple_of(g * group_rows + first * SUB, SUB)
            work = works[h].at[pl.ds(here, count * SUB), :]
            a_rows = aff.at[pl.ds(where, count * SUB), :]
            e_rows = exp.at[pl.ds(where, count * SUB), :]
            mrows = pl.ds(pl.multiple_of((h * part + g) * SUB, SUB), SUB)
            live = nlive[mrows, :] - first
            peak = peaks[mrows, :]
            for b in range(count):
                for s in range(SUB):
                    work[pl.ds(b * SUB + s, 1), :] = table[pl.ds(picked(gidx, s * blocks + b, h * part + g + first * groups), 1), :]
                now = pl.ds(b * SUB, SUB)
                v = (a_rows[now, :] - e_rows[now, :] * work[now, :]) * 2.0
                v = jnp.where(live > b, v, DEAD)
                work[now, :] = v
                peak = jnp.maximum(peak, v)
            peaks[mrows, :] = peak

        def start_bisection(h):
            for g in range(part):
                rows = pl.ds((h * part + g) * SUB, SUB)
                up[rows, :] = jnp.broadcast_to(jnp.max(peaks[rows, :], axis=1, keepdims=True), (SUB, BLOCK))
                lo[rows, :] = zero

        def fill_sums(h, q, *only):
            work = works[h].at[pl.ds(pl.multiple_of(q * (quarter * group_rows), SUB), quarter * group_rows), :]
            m0 = pl.multiple_of((h * part + q * quarter) * SUB, SUB)
            s0 = pl.multiple_of(q * (quarter * SUB), SUB)
            for g in only or range(quarter):
                rows = pl.ds(m0 + g * SUB, SUB)
                mid = (lo[rows, :] + up[rows, :]) * 0.5
                a = [None, None]
                for b in range(blocks):
                    v = jnp.clip(work[pl.ds(g * group_rows + b * SUB, SUB), :] - mid, 0.0, 1.0)
                    a[b % 2] = v if a[b % 2] is None else a[b % 2] + v
                sums[pl.ds(s0 + g * SUB, SUB), :] = a[0] + a[1]

        def lane_sums(q):
            s0 = pl.multiple_of(q * (quarter * SUB), SUB)
            return [jnp.sum(sums[pl.ds(s0 + g * SUB, SUB), :], axis=1, keepdims=True) for g in range(quarter)]

        def decide(h, q, fills):
            m0 = pl.multiple_of((h * part + q * quarter) * SUB, SUB)
            for g in range(quarter):
                rows = pl.ds(m0 + g * SUB, SUB)
                bigger = jnp.broadcast_to(fills[g], (SUB, BLOCK)) > 1.0
                low = lo[rows, :]
                high = up[rows, :]
                mid = (low + high) * 0.5
                lo[rows, :] = jnp.where(bigger, mid, low)
                up[rows, :] = jnp.where(bigger, high, mid)

        def bisect(h, beside):
            fill_sums(h, 0)

            def half_step(k):
                q = k % 2
                fills = lane_sums(q)
                steps = beside(k // 2, q)
                for g in range(quarter):
                    fill_sums(h, 1 - q, g)
                    for at, step in steps:
                        if at == g:
                            step()
                decide(h, q, fills)

            loop(0, 2 * BISECT, half_step)

        def allocate(h, g):
            rows = pl.multiple_of((h * part + g) * group_rows, SUB)
            here = pl.multiple_of(g * group_rows, SUB)
            mrows = pl.ds(pl.multiple_of((h * part + g) * SUB, SUB), SUB)
            th = up[mrows, :]
            live = nlive[mrows, :]
            for b in range(blocks):
                now = pl.ds(here + b * SUB, SUB)
                x = jnp.where(live > b, jnp.clip(works[h][now, :] - th, 0.0, 1.0), 0.0)
                if second:
                    primal[pl.ds(rows + b * SUB, SUB), :] = x
                works[h][now, :] = exp[pl.ds(rows + b * SUB, SUB), :] * x

        def scatter(h, g, first, count, parity=0):
            here = g * group_rows + first
            work = works[h]
            for s in range(count):
                where = [picked(sidx, s * blocks + b, h * part + g + first * blocks * groups) for b in range(blocks)]
                acc = accs[(s + parity) % 2]
                added = [acc[pl.ds(i, 1), :] + work[pl.ds(here + b * SUB + s, 1), :] for b, i in enumerate(where)]
                for i, v in zip(where, added):
                    acc[pl.ds(i, 1), :] = v

        for g in range(groups):
            peaks[pl.ds(g * SUB, SUB), :] = dead
        ids_in[0].wait()
        for k in range(pieces):
            for load in loads[k]:
                load.wait()
            loop(k * (part // pieces), (k + 1) * (part // pieces), lambda g: gather(0, g, 0, blocks))
        start_bisection(0)
        for load in loads[pieces]:
            load.wait()
        bisect(0, lambda g, q: [(quarter - 1, lambda: gather(1, g, q * (blocks // 2), blocks // 2)),
                                (quarter - 1, lambda: clear((2 * g + q) * per_step, per_step))])

        start_bisection(1)
        loop(0, part, lambda g: allocate(0, g))
        if second:
            stores = [pltpu.make_async_copy(
                primal.at[pl.ds(h * part_rows, part_rows), :],
                primal_out.at[pl.ds(h * part_rows, part_rows), :], sem_out.at[h]) for h in range(2)]
            stores[0].start()
        ids_in[1].wait()
        @pl.when(fits)
        def _():
            bisect(1, lambda g, q: [(2 * m, lambda m=m: scatter(0, g, q * (SUB // 2) + m, 1, m)) for m in range(SUB // 2)])

        @pl.when(jnp.logical_not(fits))
        def _():
            bisect(1, lambda g, q: [])

        loop(0, part, lambda g: allocate(1, g))
        if second:
            stores[1].start()

        @pl.when(fits)
        def _():
            loop(0, part, lambda g: scatter(1, g, 0, SUB))

        @pl.when(jnp.logical_not(fits))
        def _():
            def one(h, k):
                g = k // group_rows
                j = k - g * group_rows
                s = j // blocks
                i = gidx[j * groups + h * part + g]
                r = g * group_rows + (j - s * blocks) * SUB + s
                acc_even[pl.ds(i, 1), :] = acc_even[pl.ds(i, 1), :] + works[h][pl.ds(r, 1), :]

            for h in range(2):
                loop(0, part_rows, lambda k: one(h, k))

        def finish(i, c):
            r = pl.multiple_of(i * SUB, SUB)
            for out, o in ((keep, 0), (send, half)):
                out[pl.ds(r, SUB), :] = (
                    (acc_even[pl.ds(r + o, SUB), :] + acc_odd[pl.ds(r + o, SUB), :])
                    + (acc_even[pl.ds(r + (full + o), SUB), :] + acc_odd[pl.ds(r + (full + o), SUB), :]))
            return c

        lax.fori_loop(0, half // SUB, finish, 0, unroll=8)

        def finish_copy(t, c):
            def more(i, c):
                r = pl.multiple_of(i * SUB, SUB)
                a = pl.multiple_of(t * full + r, SUB)
                for out, o in ((keep, 0), (send, half)):
                    out[pl.ds(r, SUB), :] += acc_even[pl.ds(a + o, SUB), :] + acc_odd[pl.ds(a + o, SUB), :]
                return c

            return lax.fori_loop(0, half // SUB, more, c, unroll=8)

        lax.fori_loop(2, used, finish_copy, 0)
        if second:
            for store in stores:
                store.wait()

    smem = pl.BlockSpec(memory_space=pltpu.SMEM)
    vmem = pl.BlockSpec(memory_space=pltpu.VMEM)
    left = pl.BlockSpec(memory_space=pltpu.HBM)
    outs = [jax.ShapeDtypeStruct((half, BLOCK), f32)] * 2
    out_specs = [vmem] * 2
    scratch = [
        pltpu.VMEM((full, BLOCK), f32),
        pltpu.VMEM((part_rows, BLOCK), f32),
        pltpu.VMEM((part_rows, BLOCK), f32),
        pltpu.VMEM((COPIES * full, BLOCK), f32),
        pltpu.VMEM((COPIES * full, BLOCK), f32),
        pltpu.VMEM((members, BLOCK), f32),
        pltpu.VMEM((members, BLOCK), f32),
        pltpu.VMEM((members, BLOCK), f32),
        pltpu.VMEM((part * SUB, BLOCK), f32),
        pltpu.VMEM((rows_all, BLOCK), f32),
        pltpu.VMEM((rows_all, BLOCK), f32),
        pltpu.SMEM((rows_all,), jnp.int32),
        pltpu.SMEM((rows_all,), jnp.int32),
        pltpu.SemaphoreType.DMA((pieces + 1, 2)),
        pltpu.SemaphoreType.DMA((2,)),
    ]
    if second:
        outs += [jax.ShapeDtypeStruct((rows_all, BLOCK), f32), jax.ShapeDtypeStruct((SUB, BLOCK), f32)]
        out_specs += [left, vmem]
        scratch += [pltpu.VMEM((rows_all, BLOCK), f32), pltpu.SemaphoreType.DMA((2,))]
    tables = [vmem] * (4 if second else 2)
    call = pl.pallas_call(
        body,
        out_shape=outs,
        in_specs=[left, left, smem] + tables + [left, left, vmem],
        out_specs=out_specs,
        scratch_shapes=scratch,
        compiler_params=pltpu.CompilerParams(vmem_limit_bytes=48 << 20),
        name="iterate2" if second else "iterate1",
    )

    def run(gidx, sidx, ncopy, *rest):
        *tables, aff, exp, nlive = rest
        aff, exp = (pltpu.with_memory_space_constraint(x, pltpu.HBM) for x in (aff, exp))
        return call(gidx, sidx, ncopy, *tables, aff, exp, nlive)

    return run


def vmem_call(body, name, *outs):
    spec = pl.BlockSpec(memory_space=pltpu.VMEM)
    return pl.pallas_call(
        body,
        out_shape=[jax.ShapeDtypeStruct(shape, jnp.float32) for shape in outs],
        out_specs=[spec] * len(outs),
        compiler_params=pltpu.CompilerParams(vmem_limit_bytes=4 << 20),
        name=name,
    )


def spread_duals(x, chips, core):
    own_rows = x.shape[0]

    def body(x, core, every):
        for p in range(chips):
            every[pl.ds(p * own_rows, own_rows), :] = x[...]

    return vmem_call(body, "spread_duals", (chips * own_rows, BLOCK))(
        x, jnp.full((SUB, BLOCK), core, jnp.int32))[0]


def sum_chips(x, chips):
    own_rows = x.shape[0] // chips

    def body(x, out):
        parts = [x[pl.ds(p * own_rows, own_rows), :] for p in range(chips)]
        while len(parts) > 1:
            parts = [a + b for a, b in zip(parts[::2], parts[1::2])]
        out[...] = parts[0]

    return vmem_call(body, "sum_chips", (own_rows, BLOCK))(x)[0]


def gradient_of(plane, shifted, limit):
    one, two, three = shifted
    return ((plane[...] + two[...]) + (one[...] + three[...])) - limit[...]


def spread_gradient(plane, shifted, limit, chips):
    own_rows = plane.shape[0]

    def body(plane, one, two, three, limit, gradient, every):
        g = gradient_of(plane, (one, two, three), limit)
        gradient[...] = g
        for p in range(chips):
            every[pl.ds(p * own_rows, own_rows), :] = g

    return vmem_call(body, "spread_gradient", plane.shape, (chips * own_rows, BLOCK))(plane, *shifted, limit)


def last_gradient(plane, shifted, limit, shards):
    def body(plane, one, two, three, limit, gradient, parts):
        g = gradient_of(plane, (one, two, three), limit)
        gradient[...] = g
        part = jnp.sum(jnp.sum(g * g, axis=0, keepdims=True), axis=1, keepdims=True)
        parts[...] = jnp.broadcast_to(part[None], parts.shape)

    return vmem_call(body, "last_gradient", plane.shape, (shards, 1, BLOCK))(plane, *shifted, limit)


def last_duals(duals, first, sumsq, second, parts, item_count):
    def body(duals, first, sumsq, second, parts, out):
        scale = jnp.sqrt(sumsq[0:1, :] / item_count + 1e-6)
        lam = jnp.maximum(duals[...] + 0.5 * first[...] / scale, 0.0)
        scale = jnp.sqrt(jnp.sum(parts[...], axis=0) / item_count + 1e-6)
        out[...] = jnp.maximum(lam + 0.5 * second[...] / scale, 0.0)

    return vmem_call(body, "last_duals", duals.shape)(duals, first, sumsq, second, parts)[0]


def local(candidates, affinity, exposure, lengths, item_limit, item_duals, *, grp_size, shard_size):
    chips = shard_size // 2
    same_core = [[2 * p + c for p in range(chips)] for c in range(2)]
    swap = [(g * shard_size + s, g * shard_size + (s ^ 1)) for g in range(grp_size) for s in range(shard_size)]
    members, slots = affinity.shape
    blocks = slots // BLOCK
    groups = members // SUB
    own_items = item_limit.shape[0]
    item_count = own_items * shard_size
    own_rows = own_items // BLOCK
    half = chips * own_rows
    full = 2 * half
    core = lax.axis_index("shard") % 2

    def swap_cores(x):
        return lax.ppermute(x, AXES, swap)

    def as_rows(x):
        return x.reshape(groups, SUB, blocks, BLOCK).transpose(0, 2, 1, 3).reshape(-1, BLOCK)

    def exchange(x):
        x = x.reshape(chips, 1, own_items)
        return lax.all_to_all(
            x, "shard", 0, 0, axis_index_groups=same_core, tiled=True).reshape(half, BLOCK)

    def gather_halves(every):
        every = exchange(every)
        return every, swap_cores(every)

    def reduce_loads(keep, send):
        chip = keep + swap_cores(send)
        plane = sum_chips(exchange(chip), chips)
        return plane, [
            lax.ppermute(plane, "grp", [(g, (g + d) % grp_size) for g in range(grp_size)])
            for d in range(1, grp_size)
        ]

    shard_of = candidates // own_rows
    gidx = (jnp.where(shard_of % 2 == core, 0, half) + (shard_of // 2) * own_rows + candidates % own_rows).reshape(-1)
    batch = gidx.reshape(-1, blocks)
    earlier = jnp.arange(blocks)[:, None] > jnp.arange(blocks)[None, :]
    copy = jnp.sum((batch[:, :, None] == batch[:, None, :]) & earlier, axis=2, dtype=jnp.int32)
    sidx = (batch + full * copy).reshape(groups, -1).T.reshape(-1)
    gidx = gidx.reshape(groups, -1).T.reshape(-1)
    ncopy = (jnp.max(copy) + 1).reshape(1)

    aff = as_rows(affinity)
    exp = as_rows(exposure)
    nlive = jnp.broadcast_to((lengths // BLOCK)[:, None], (members, BLOCK))
    limit = item_limit.reshape(own_rows, BLOCK)
    duals = item_duals.reshape(own_rows, BLOCK)

    own_d, other_d = gather_halves(spread_duals(duals, chips, core))
    keep, send = iteration_kernel(False, groups, blocks, half, item_count)(
        gidx, sidx, ncopy, own_d, other_d, aff, exp, nlive)
    first, every = spread_gradient(*reduce_loads(keep, send), limit, chips)

    own_g, other_g = gather_halves(every)
    keep, send, primal, sumsq = iteration_kernel(True, groups, blocks, half, item_count)(
        gidx, sidx, ncopy, own_d, other_d, own_g, other_g, aff, exp, nlive)
    second, parts = last_gradient(*reduce_loads(keep, send), limit, shard_size)
    parts = lax.all_to_all(parts, "shard", 0, 0, tiled=True)
    duals = last_duals(duals, first, sumsq, second, parts, item_count)

    primal = primal.reshape(groups, blocks, SUB, BLOCK).transpose(0, 2, 1, 3).reshape(members, slots)
    return primal, duals.reshape(-1)


def solution(mesh):
    placed = (
        P(("grp", "shard"), None),
        P(("grp", "shard"), None),
        P(("grp", "shard"), None),
        P(("grp", "shard")),
        P("shard"),
        P("shard"),
    )

    def run(*args):
        return local(*args, grp_size=mesh.shape["grp"], shard_size=mesh.shape["shard"])

    return jax.shard_map(
        run,
        mesh=mesh,
        in_specs=placed,
        out_specs=(P(("grp", "shard"), None), P("shard")),
        check_vma=False,
    )
```

```python
import jax
import jax.numpy as jnp
from jax import lax
from jax.experimental import pallas as pl
from jax.experimental.pallas import tpu as pltpu
from jax.sharding import PartitionSpec as P

BLOCK = 128
BISECT = 16
SUB = 8
COPIES = 8
DEAD = -1e30

AXES = ("grp", "shard")


def iteration_kernel(second, groups, blocks, half, item_count):
    full = 2 * half
    members = groups * SUB
    group_rows = SUB * blocks
    rows_all = groups * group_rows
    part = groups // 2
    quarter = part // 2
    part_rows = part * group_rows
    assert quarter * 4 == groups and part == BISECT and blocks % 2 == 0
    pieces = 4
    f32 = jnp.float32

    def body(*refs):
        if second:
            (gidx_in, sidx_in, ncopy, own_d, other_d, own_g, other_g, aff_in, exp_in, nlive,
             keep, send, primal_out, sumsq,
             table, work_a, work_b, acc_even, acc_odd, lo, up, peaks, sums, aff, exp, gidx, sidx, sem_in, sem_id,
             primal, sem_out) = refs
        else:
            (gidx_in, sidx_in, ncopy, own_d, other_d, aff_in, exp_in, nlive,
             keep, send,
             table, work_a, work_b, acc_even, acc_odd, lo, up, peaks, sums, aff, exp, gidx, sidx, sem_in, sem_id) = refs
        works = (work_a, work_b)
        accs = (acc_even, acc_odd)

        ids_in = [pltpu.make_async_copy(src, dst, sem_id.at[k])
                  for k, (src, dst) in enumerate(((gidx_in, gidx), (sidx_in, sidx)))]
        size = part_rows // pieces
        spans = [(k * size, size) for k in range(pieces)] + [(part_rows, part_rows)]
        loads = [[pltpu.make_async_copy(src.at[pl.ds(r, n), :], dst.at[pl.ds(r, n), :], sem_in.at[k, j])
                  for j, (src, dst) in enumerate(((aff_in, aff), (exp_in, exp)))]
                 for k, (r, n) in enumerate(spans)]
        ids_in[0].start()
        for pair in loads:
            for load in pair:
                load.start()
        ids_in[1].start()

        if second:
            def square(i, s):
                r = pl.multiple_of(i * SUB, SUB)
                a = own_g[pl.ds(r, SUB), :]
                b = other_g[pl.ds(r, SUB), :]
                return s + (a * a + b * b)

            s = lax.fori_loop(0, half // SUB, square, jnp.zeros((SUB, BLOCK), f32), unroll=8)
            total = jnp.sum(jnp.sum(s, axis=1, keepdims=True), axis=0, keepdims=True)
            total = jnp.broadcast_to(total, (SUB, BLOCK))
            sumsq[...] = total
            scale = jnp.sqrt(total / item_count + 1e-6)

            def fill_table(i, c):
                r = pl.multiple_of(i * SUB, SUB)
                for d, g, off in ((own_d, own_g, 0), (other_d, other_g, half)):
                    table[pl.ds(r + off, SUB), :] = jnp.maximum(
                        d[pl.ds(r, SUB), :] + 0.5 * g[pl.ds(r, SUB), :] / scale, 0.0)
                return c
        else:
            def fill_table(i, c):
                r = pl.multiple_of(i * SUB, SUB)
                table[pl.ds(r, SUB), :] = own_d[pl.ds(r, SUB), :]
                table[pl.ds(r + half, SUB), :] = other_d[pl.ds(r, SUB), :]
                return c

        lax.fori_loop(0, half // SUB, fill_table, 0, unroll=8)

        n = ncopy[0]
        fits = n <= COPIES
        used = jnp.where(fits, jnp.maximum(n, 2), 2)
        zero = jnp.zeros((SUB, BLOCK), f32)
        dead = jnp.full((SUB, BLOCK), DEAD, f32)
        vregs = full // SUB
        per_step = vregs // (2 * BISECT)
        assert per_step * 2 * BISECT <= vregs and vregs % 16 == 0

        def clear(first, count):
            for acc in accs:
                some = acc.at[pl.ds(pl.multiple_of(first * SUB, SUB), count * SUB), :]
                for i in range(count):
                    some[pl.ds(i * SUB, SUB), :] = zero

        def clear_16(i, c):
            clear(16 * i, 16)
            return c

        lax.fori_loop(vregs // 16, used * vregs // 16, clear_16, 0)
        clear(per_step * 2 * BISECT, vregs - per_step * 2 * BISECT)

        def loop(first, last, f):
            def trip(i, c):
                f(i)
                return c

            lax.fori_loop(first, last, trip, 0)

        def picked(ids, j, g):
            return ids.at[pl.ds(j * groups, rows_all - j * groups)][g]

        def gather(h, g, first, count):
            rows = (h * part + g) * group_rows
            where = pl.multiple_of(rows + first * SUB, SUB)
            here = pl.multiple_of(g * group_rows + first * SUB, SUB)
            work = works[h].at[pl.ds(here, count * SUB), :]
            a_rows = aff.at[pl.ds(where, count * SUB), :]
            e_rows = exp.at[pl.ds(where, count * SUB), :]
            mrows = pl.ds(pl.multiple_of((h * part + g) * SUB, SUB), SUB)
            live = nlive[mrows, :] - first
            peak = peaks[mrows, :]
            for b in range(count):
                for s in range(SUB):
                    work[pl.ds(b * SUB + s, 1), :] = table[pl.ds(picked(gidx, s * blocks + b, h * part + g + first * groups), 1), :]
                now = pl.ds(b * SUB, SUB)
                v = (a_rows[now, :] - e_rows[now, :] * work[now, :]) * 2.0
                v = jnp.where(live > b, v, DEAD)
                work[now, :] = v
                peak = jnp.maximum(peak, v)
            peaks[mrows, :] = peak

        def start_bisection(h):
            for g in range(part):
                rows = pl.ds((h * part + g) * SUB, SUB)
                up[rows, :] = jnp.broadcast_to(jnp.max(peaks[rows, :], axis=1, keepdims=True), (SUB, BLOCK))
                lo[rows, :] = zero

        def fill_sums(h, q, *only):
            work = works[h].at[pl.ds(pl.multiple_of(q * (quarter * group_rows), SUB), quarter * group_rows), :]
            m0 = pl.multiple_of((h * part + q * quarter) * SUB, SUB)
            s0 = pl.multiple_of(q * (quarter * SUB), SUB)
            for g in only or range(quarter):
                rows = pl.ds(m0 + g * SUB, SUB)
                mid = (lo[rows, :] + up[rows, :]) * 0.5
                a = [None, None]
                for b in range(blocks):
                    v = jnp.clip(work[pl.ds(g * group_rows + b * SUB, SUB), :] - mid, 0.0, 1.0)
                    a[b % 2] = v if a[b % 2] is None else a[b % 2] + v
                sums[pl.ds(s0 + g * SUB, SUB), :] = a[0] + a[1]

        def lane_sums(q):
            s0 = pl.multiple_of(q * (quarter * SUB), SUB)
            return [jnp.sum(sums[pl.ds(s0 + g * SUB, SUB), :], axis=1, keepdims=True) for g in range(quarter)]

        def decide(h, q, fills):
            m0 = pl.multiple_of((h * part + q * quarter) * SUB, SUB)
            for g in range(quarter):
                rows = pl.ds(m0 + g * SUB, SUB)
                bigger = jnp.broadcast_to(fills[g], (SUB, BLOCK)) > 1.0
                low = lo[rows, :]
                high = up[rows, :]
                mid = (low + high) * 0.5
                lo[rows, :] = jnp.where(bigger, mid, low)
                up[rows, :] = jnp.where(bigger, high, mid)

        def bisect(h, beside):
            fill_sums(h, 0)

            def half_step(k):
                q = k % 2
                fills = lane_sums(q)
                steps = beside(k // 2, q)
                for g in range(quarter):
                    fill_sums(h, 1 - q, g)
                    for at, step in steps:
                        if at == g:
                            step()
                decide(h, q, fills)

            loop(0, 2 * BISECT, half_step)

        def allocate(h, g):
            rows = pl.multiple_of((h * part + g) * group_rows, SUB)
            here = pl.multiple_of(g * group_rows, SUB)
            mrows = pl.ds(pl.multiple_of((h * part + g) * SUB, SUB), SUB)
            th = up[mrows, :]
            live = nlive[mrows, :]
            for b in range(blocks):
                now = pl.ds(here + b * SUB, SUB)
                x = jnp.where(live > b, jnp.clip(works[h][now, :] - th, 0.0, 1.0), 0.0)
                if second:
                    primal[pl.ds(rows + b * SUB, SUB), :] = x
                works[h][now, :] = exp[pl.ds(rows + b * SUB, SUB), :] * x

        def scatter(h, g, first, count, parity=0):
            here = g * group_rows + first
            work = works[h]
            for s in range(count):
                where = [picked(sidx, s * blocks + b, h * part + g + first * blocks * groups) for b in range(blocks)]
                acc = accs[(s + parity) % 2]
                added = [acc[pl.ds(i, 1), :] + work[pl.ds(here + b * SUB + s, 1), :] for b, i in enumerate(where)]
                for i, v in zip(where, added):
                    acc[pl.ds(i, 1), :] = v

        for g in range(groups):
            peaks[pl.ds(g * SUB, SUB), :] = dead
        ids_in[0].wait()
        for k in range(pieces):
            for load in loads[k]:
                load.wait()
            loop(k * (part // pieces), (k + 1) * (part // pieces), lambda g: gather(0, g, 0, blocks))
        start_bisection(0)
        for load in loads[pieces]:
            load.wait()
        bisect(0, lambda g, q: [(quarter - 1, lambda: gather(1, g, q * (blocks // 2), blocks // 2)),
                                (quarter - 1, lambda: clear((2 * g + q) * per_step, per_step))])

        start_bisection(1)
        loop(0, part, lambda g: allocate(0, g))
        if second:
            stores = [pltpu.make_async_copy(
                primal.at[pl.ds(h * part_rows, part_rows), :],
                primal_out.at[pl.ds(h * part_rows, part_rows), :], sem_out.at[h]) for h in range(2)]
            stores[0].start()
        ids_in[1].wait()
        @pl.when(fits)
        def _():
            bisect(1, lambda g, q: [(2 * m, lambda m=m: scatter(0, g, q * (SUB // 2) + m, 1, m)) for m in range(SUB // 2)])

        @pl.when(jnp.logical_not(fits))
        def _():
            bisect(1, lambda g, q: [])

        loop(0, part, lambda g: allocate(1, g))
        if second:
            stores[1].start()

        @pl.when(fits)
        def _():
            loop(0, part, lambda g: scatter(1, g, 0, SUB))

        @pl.when(jnp.logical_not(fits))
        def _():
            def one(h, k):
                g = k // group_rows
                j = k - g * group_rows
                s = j // blocks
                i = gidx[j * groups + h * part + g]
                r = g * group_rows + (j - s * blocks) * SUB + s
                acc_even[pl.ds(i, 1), :] = acc_even[pl.ds(i, 1), :] + works[h][pl.ds(r, 1), :]

            for h in range(2):
                loop(0, part_rows, lambda k: one(h, k))

        def finish(i, c):
            r = pl.multiple_of(i * SUB, SUB)
            for out, o in ((keep, 0), (send, half)):
                out[pl.ds(r, SUB), :] = (
                    (acc_even[pl.ds(r + o, SUB), :] + acc_odd[pl.ds(r + o, SUB), :])
                    + (acc_even[pl.ds(r + (full + o), SUB), :] + acc_odd[pl.ds(r + (full + o), SUB), :]))
            return c

        lax.fori_loop(0, half // SUB, finish, 0, unroll=8)

        def finish_copy(t, c):
            def more(i, c):
                r = pl.multiple_of(i * SUB, SUB)
                a = pl.multiple_of(t * full + r, SUB)
                for out, o in ((keep, 0), (send, half)):
                    out[pl.ds(r, SUB), :] += acc_even[pl.ds(a + o, SUB), :] + acc_odd[pl.ds(a + o, SUB), :]
                return c

            return lax.fori_loop(0, half // SUB, more, c, unroll=8)

        lax.fori_loop(2, used, finish_copy, 0)
        if second:
            for store in stores:
                store.wait()

    smem = pl.BlockSpec(memory_space=pltpu.SMEM)
    vmem = pl.BlockSpec(memory_space=pltpu.VMEM)
    left = pl.BlockSpec(memory_space=pltpu.HBM)
    outs = [jax.ShapeDtypeStruct((half, BLOCK), f32)] * 2
    out_specs = [vmem] * 2
    scratch = [
        pltpu.VMEM((full, BLOCK), f32),
        pltpu.VMEM((part_rows, BLOCK), f32),
        pltpu.VMEM((part_rows, BLOCK), f32),
        pltpu.VMEM((COPIES * full, BLOCK), f32),
        pltpu.VMEM((COPIES * full, BLOCK), f32),
        pltpu.VMEM((members, BLOCK), f32),
        pltpu.VMEM((members, BLOCK), f32),
        pltpu.VMEM((members, BLOCK), f32),
        pltpu.VMEM((part * SUB, BLOCK), f32),
        pltpu.VMEM((rows_all, BLOCK), f32),
        pltpu.VMEM((rows_all, BLOCK), f32),
        pltpu.SMEM((rows_all,), jnp.int32),
        pltpu.SMEM((rows_all,), jnp.int32),
        pltpu.SemaphoreType.DMA((pieces + 1, 2)),
        pltpu.SemaphoreType.DMA((2,)),
    ]
    if second:
        outs += [jax.ShapeDtypeStruct((rows_all, BLOCK), f32), jax.ShapeDtypeStruct((SUB, BLOCK), f32)]
        out_specs += [left, vmem]
        scratch += [pltpu.VMEM((rows_all, BLOCK), f32), pltpu.SemaphoreType.DMA((2,))]
    tables = [vmem] * (4 if second else 2)
    call = pl.pallas_call(
        body,
        out_shape=outs,
        in_specs=[left, left, smem] + tables + [left, left, vmem],
        out_specs=out_specs,
        scratch_shapes=scratch,
        compiler_params=pltpu.CompilerParams(vmem_limit_bytes=48 << 20),
        name="iterate2" if second else "iterate1",
    )

    def run(gidx, sidx, ncopy, *rest):
        *tables, aff, exp, nlive = rest
        aff, exp = (pltpu.with_memory_space_constraint(x, pltpu.HBM) for x in (aff, exp))
        return call(gidx, sidx, ncopy, *tables, aff, exp, nlive)

    return run


def vmem_call(body, name, *outs):
    spec = pl.BlockSpec(memory_space=pltpu.VMEM)
    return pl.pallas_call(
        body,
        out_shape=[jax.ShapeDtypeStruct(shape, jnp.float32) for shape in outs],
        out_specs=[spec] * len(outs),
        compiler_params=pltpu.CompilerParams(vmem_limit_bytes=4 << 20),
        name=name,
    )


def spread_duals(x, chips, core):
    own_rows = x.shape[0]

    def body(x, core, every):
        for p in range(chips):
            every[pl.ds(p * own_rows, own_rows), :] = x[...]

    return vmem_call(body, "spread_duals", (chips * own_rows, BLOCK))(
        x, jnp.full((SUB, BLOCK), core, jnp.int32))[0]


def sum_chips(x, chips):
    own_rows = x.shape[0] // chips

    def body(x, out):
        parts = [x[pl.ds(p * own_rows, own_rows), :] for p in range(chips)]
        while len(parts) > 1:
            parts = [a + b for a, b in zip(parts[::2], parts[1::2])]
        out[...] = parts[0]

    return vmem_call(body, "sum_chips", (own_rows, BLOCK))(x)[0]


def gradient_of(plane, shifted, limit):
    two, one, three = shifted
    return ((plane[...] + two[...]) + (one[...] + three[...])) - limit[...]


def spread_gradient(plane, shifted, limit, chips):
    own_rows = plane.shape[0]

    def body(plane, two, one, three, limit, gradient, every):
        g = gradient_of(plane, (two, one, three), limit)
        gradient[...] = g
        for p in range(chips):
            every[pl.ds(p * own_rows, own_rows), :] = g

    return vmem_call(body, "spread_gradient", plane.shape, (chips * own_rows, BLOCK))(plane, *shifted, limit)


def last_gradient(plane, shifted, limit, shards):
    def body(plane, two, one, three, limit, gradient, parts):
        g = gradient_of(plane, (two, one, three), limit)
        gradient[...] = g
        part = jnp.sum(jnp.sum(g * g, axis=0, keepdims=True), axis=1, keepdims=True)
        parts[...] = jnp.broadcast_to(part[None], parts.shape)

    return vmem_call(body, "last_gradient", plane.shape, (shards, 1, BLOCK))(plane, *shifted, limit)


def last_duals(duals, first, sumsq, second, parts, item_count):
    def body(duals, first, sumsq, second, parts, out):
        scale = jnp.sqrt(sumsq[0:1, :] / item_count + 1e-6)
        lam = jnp.maximum(duals[...] + 0.5 * first[...] / scale, 0.0)
        scale = jnp.sqrt(jnp.sum(parts[...], axis=0) / item_count + 1e-6)
        out[...] = jnp.maximum(lam + 0.5 * second[...] / scale, 0.0)

    return vmem_call(body, "last_duals", duals.shape)(duals, first, sumsq, second, parts)[0]


def local(candidates, affinity, exposure, lengths, item_limit, item_duals, *, grp_size, shard_size):
    chips = shard_size // 2
    same_core = [[2 * p + c for p in range(chips)] for c in range(2)]
    swap = [(g * shard_size + s, g * shard_size + (s ^ 1)) for g in range(grp_size) for s in range(shard_size)]
    members, slots = affinity.shape
    blocks = slots // BLOCK
    groups = members // SUB
    own_items = item_limit.shape[0]
    item_count = own_items * shard_size
    own_rows = own_items // BLOCK
    half = chips * own_rows
    full = 2 * half
    core = lax.axis_index("shard") % 2

    def swap_cores(x):
        return lax.ppermute(x, AXES, swap)

    def as_rows(x):
        return x.reshape(groups, SUB, blocks, BLOCK).transpose(0, 2, 1, 3).reshape(-1, BLOCK)

    def exchange(x):
        x = x.reshape(chips, 1, own_items)
        return lax.all_to_all(
            x, "shard", 0, 0, axis_index_groups=same_core, tiled=True).reshape(half, BLOCK)

    def gather_halves(every):
        every = exchange(every)
        return every, swap_cores(every)

    def reduce_loads(keep, send):
        chip = keep + swap_cores(send)
        plane = sum_chips(exchange(chip), chips)
        return plane, [
            lax.ppermute(plane, "grp", [(g, (g + d) % grp_size) for g in range(grp_size)])
            for d in (2, 1, 3)
        ]

    shard_of = candidates // own_rows
    gidx = (jnp.where(shard_of % 2 == core, 0, half) + (shard_of // 2) * own_rows + candidates % own_rows).reshape(-1)
    batch = gidx.reshape(-1, blocks)
    earlier = jnp.arange(blocks)[:, None] > jnp.arange(blocks)[None, :]
    copy = jnp.sum((batch[:, :, None] == batch[:, None, :]) & earlier, axis=2, dtype=jnp.int32)
    sidx = (batch + full * copy).reshape(groups, -1).T.reshape(-1)
    gidx = gidx.reshape(groups, -1).T.reshape(-1)
    ncopy = (jnp.max(copy) + 1).reshape(1)

    aff = as_rows(affinity)
    exp = as_rows(exposure)
    nlive = jnp.broadcast_to((lengths // BLOCK)[:, None], (members, BLOCK))
    limit = item_limit.reshape(own_rows, BLOCK)
    duals = item_duals.reshape(own_rows, BLOCK)

    own_d, other_d = gather_halves(spread_duals(duals, chips, core))
    keep, send = iteration_kernel(False, groups, blocks, half, item_count)(
        gidx, sidx, ncopy, own_d, other_d, aff, exp, nlive)
    first, every = spread_gradient(*reduce_loads(keep, send), limit, chips)

    own_g, other_g = gather_halves(every)
    keep, send, primal, sumsq = iteration_kernel(True, groups, blocks, half, item_count)(
        gidx, sidx, ncopy, own_d, other_d, own_g, other_g, aff, exp, nlive)
    second, parts = last_gradient(*reduce_loads(keep, send), limit, shard_size)
    parts = lax.all_to_all(parts, "shard", 0, 0, tiled=True)
    duals = last_duals(duals, first, sumsq, second, parts, item_count)

    primal = primal.reshape(groups, blocks, SUB, BLOCK).transpose(0, 2, 1, 3).reshape(members, slots)
    return primal, duals.reshape(-1)


def solution(mesh):
    placed = (
        P(("grp", "shard"), None),
        P(("grp", "shard"), None),
        P(("grp", "shard"), None),
        P(("grp", "shard")),
        P("shard"),
        P("shard"),
    )

    def run(*args):
        return local(*args, grp_size=mesh.shape["grp"], shard_size=mesh.shape["shard"])

    return jax.shard_map(
        run,
        mesh=mesh,
        in_specs=placed,
        out_specs=(P(("grp", "shard"), None), P("shard")),
        check_vma=False,
    )
```

```python
import jax
import jax.numpy as jnp
from jax import lax
from jax.experimental import pallas as pl
from jax.experimental.pallas import tpu as pltpu
from jax.sharding import PartitionSpec as P

BLOCK = 128
BISECT = 16
SUB = 8
COPIES = 8
DEAD = -1e30

AXES = ("grp", "shard")


def iteration_kernel(second, groups, blocks, half, item_count):
    full = 2 * half
    members = groups * SUB
    group_rows = SUB * blocks
    rows_all = groups * group_rows
    part = groups // 2
    quarter = part // 2
    part_rows = part * group_rows
    assert quarter * 4 == groups and part == BISECT and blocks % 2 == 0
    pieces = 4
    f32 = jnp.float32

    def body(*refs):
        if second:
            (gidx_in, sidx_in, ncopy, own_d, other_d, own_g, other_g, aff_in, exp_in, nlive,
             keep, send, primal_out, sumsq,
             table, work_a, work_b, acc_even, acc_odd, lo, up, peaks, sums, aff, exp, gidx, sidx, sem_in, sem_id,
             primal, sem_out) = refs
        else:
            (gidx_in, sidx_in, ncopy, own_d, other_d, aff_in, exp_in, nlive,
             keep, send,
             table, work_a, work_b, acc_even, acc_odd, lo, up, peaks, sums, aff, exp, gidx, sidx, sem_in, sem_id) = refs
        works = (work_a, work_b)
        accs = (acc_even, acc_odd)

        ids_in = [pltpu.make_async_copy(src, dst, sem_id.at[k])
                  for k, (src, dst) in enumerate(((gidx_in, gidx), (sidx_in, sidx)))]
        size = part_rows // pieces
        spans = [(k * size, size) for k in range(pieces)] + [(part_rows, part_rows)]
        loads = [[pltpu.make_async_copy(src.at[pl.ds(r, n), :], dst.at[pl.ds(r, n), :], sem_in.at[k, j])
                  for j, (src, dst) in enumerate(((aff_in, aff), (exp_in, exp)))]
                 for k, (r, n) in enumerate(spans)]
        ids_in[0].start()
        for pair in loads:
            for load in pair:
                load.start()
        ids_in[1].start()

        if second:
            def square(i, s):
                r = pl.multiple_of(i * SUB, SUB)
                a = own_g[pl.ds(r, SUB), :]
                b = other_g[pl.ds(r, SUB), :]
                return s + (a * a + b * b)

            s = lax.fori_loop(0, half // SUB, square, jnp.zeros((SUB, BLOCK), f32), unroll=8)
            total = jnp.sum(jnp.sum(s, axis=1, keepdims=True), axis=0, keepdims=True)
            total = jnp.broadcast_to(total, (SUB, BLOCK))
            sumsq[...] = total
            step = 0.5 / jnp.sqrt(total / item_count + 1e-6)

            def fill_table(i, c):
                r = pl.multiple_of(i * SUB, SUB)
                for d, g, off in ((own_d, own_g, 0), (other_d, other_g, half)):
                    table[pl.ds(r + off, SUB), :] = jnp.maximum(
                        d[pl.ds(r, SUB), :] + g[pl.ds(r, SUB), :] * step, 0.0)
                return c
        else:
            def fill_table(i, c):
                r = pl.multiple_of(i * SUB, SUB)
                table[pl.ds(r, SUB), :] = own_d[pl.ds(r, SUB), :]
                table[pl.ds(r + half, SUB), :] = other_d[pl.ds(r, SUB), :]
                return c

        lax.fori_loop(0, half // SUB, fill_table, 0, unroll=8)

        n = ncopy[0]
        fits = n <= COPIES
        used = jnp.where(fits, jnp.maximum(n, 2), 2)
        zero = jnp.zeros((SUB, BLOCK), f32)
        dead = jnp.full((SUB, BLOCK), DEAD, f32)
        vregs = full // SUB
        per_step = vregs // (2 * BISECT)
        assert per_step * 2 * BISECT <= vregs and vregs % 16 == 0

        def clear(first, count):
            for acc in accs:
                some = acc.at[pl.ds(pl.multiple_of(first * SUB, SUB), count * SUB), :]
                for i in range(count):
                    some[pl.ds(i * SUB, SUB), :] = zero

        def clear_16(i, c):
            clear(16 * i, 16)
            return c

        lax.fori_loop(vregs // 16, used * vregs // 16, clear_16, 0)
        clear(per_step * 2 * BISECT, vregs - per_step * 2 * BISECT)

        def loop(first, last, f):
            def trip(i, c):
                f(i)
                return c

            lax.fori_loop(first, last, trip, 0)

        def picked(ids, j, g):
            return ids.at[pl.ds(j * groups, rows_all - j * groups)][g]

        def gather(h, g, first, count):
            rows = (h * part + g) * group_rows
            where = pl.multiple_of(rows + first * SUB, SUB)
            here = pl.multiple_of(g * group_rows + first * SUB, SUB)
            work = works[h].at[pl.ds(here, count * SUB), :]
            a_rows = aff.at[pl.ds(where, count * SUB), :]
            e_rows = exp.at[pl.ds(where, count * SUB), :]
            mrows = pl.ds(pl.multiple_of((h * part + g) * SUB, SUB), SUB)
            live = nlive[mrows, :] - first
            peak = peaks[mrows, :]
            for b in range(count):
                for s in range(SUB):
                    work[pl.ds(b * SUB + s, 1), :] = table[pl.ds(picked(gidx, s * blocks + b, h * part + g + first * groups), 1), :]
                now = pl.ds(b * SUB, SUB)
                v = (a_rows[now, :] - e_rows[now, :] * work[now, :]) * 2.0
                v = jnp.where(live > b, v, DEAD)
                work[now, :] = v
                peak = jnp.maximum(peak, v)
            peaks[mrows, :] = peak

        def start_bisection(h):
            for g in range(part):
                rows = pl.ds((h * part + g) * SUB, SUB)
                up[rows, :] = jnp.broadcast_to(jnp.max(peaks[rows, :], axis=1, keepdims=True), (SUB, BLOCK))
                lo[rows, :] = zero

        def fill_sums(h, q, *only):
            work = works[h].at[pl.ds(pl.multiple_of(q * (quarter * group_rows), SUB), quarter * group_rows), :]
            m0 = pl.multiple_of((h * part + q * quarter) * SUB, SUB)
            s0 = pl.multiple_of(q * (quarter * SUB), SUB)
            for g in only or range(quarter):
                rows = pl.ds(m0 + g * SUB, SUB)
                mid = (lo[rows, :] + up[rows, :]) * 0.5
                a = [None, None]
                for b in range(blocks):
                    v = jnp.clip(work[pl.ds(g * group_rows + b * SUB, SUB), :] - mid, 0.0, 1.0)
                    a[b % 2] = v if a[b % 2] is None else a[b % 2] + v
                sums[pl.ds(s0 + g * SUB, SUB), :] = a[0] + a[1]

        def lane_sums(q):
            s0 = pl.multiple_of(q * (quarter * SUB), SUB)
            return [jnp.sum(sums[pl.ds(s0 + g * SUB, SUB), :], axis=1, keepdims=True) for g in range(quarter)]

        def decide(h, q, fills):
            m0 = pl.multiple_of((h * part + q * quarter) * SUB, SUB)
            for g in range(quarter):
                rows = pl.ds(m0 + g * SUB, SUB)
                bigger = jnp.broadcast_to(fills[g], (SUB, BLOCK)) > 1.0
                low = lo[rows, :]
                high = up[rows, :]
                mid = (low + high) * 0.5
                lo[rows, :] = jnp.where(bigger, mid, low)
                up[rows, :] = jnp.where(bigger, high, mid)

        def bisect(h, beside):
            fill_sums(h, 0)

            def half_step(k):
                q = k % 2
                fills = lane_sums(q)
                steps = beside(k // 2, q)
                for g in range(quarter):
                    fill_sums(h, 1 - q, g)
                    for at, step in steps:
                        if at == g:
                            step()
                decide(h, q, fills)

            loop(0, 2 * BISECT, half_step)

        def allocate(h, g):
            rows = pl.multiple_of((h * part + g) * group_rows, SUB)
            here = pl.multiple_of(g * group_rows, SUB)
            mrows = pl.ds(pl.multiple_of((h * part + g) * SUB, SUB), SUB)
            th = up[mrows, :]
            live = nlive[mrows, :]
            for b in range(blocks):
                now = pl.ds(here + b * SUB, SUB)
                x = jnp.where(live > b, jnp.clip(works[h][now, :] - th, 0.0, 1.0), 0.0)
                if second:
                    primal[pl.ds(rows + b * SUB, SUB), :] = x
                works[h][now, :] = exp[pl.ds(rows + b * SUB, SUB), :] * x

        def scatter(h, g, first, count, parity=0):
            here = g * group_rows + first
            work = works[h]
            for s in range(count):
                where = [picked(sidx, s * blocks + b, h * part + g + first * blocks * groups) for b in range(blocks)]
                acc = accs[(s + parity) % 2]
                added = [acc[pl.ds(i, 1), :] + work[pl.ds(here + b * SUB + s, 1), :] for b, i in enumerate(where)]
                for i, v in zip(where, added):
                    acc[pl.ds(i, 1), :] = v

        for g in range(groups):
            peaks[pl.ds(g * SUB, SUB), :] = dead
        ids_in[0].wait()
        for k in range(pieces):
            for load in loads[k]:
                load.wait()
            loop(k * (part // pieces), (k + 1) * (part // pieces), lambda g: gather(0, g, 0, blocks))
        start_bisection(0)
        for load in loads[pieces]:
            load.wait()
        bisect(0, lambda g, q: [(quarter - 1, lambda: gather(1, g, q * (blocks // 2), blocks // 2)),
                                (quarter - 1, lambda: clear((2 * g + q) * per_step, per_step))])

        start_bisection(1)
        loop(0, part, lambda g: allocate(0, g))
        if second:
            stores = [pltpu.make_async_copy(
                primal.at[pl.ds(h * part_rows, part_rows), :],
                primal_out.at[pl.ds(h * part_rows, part_rows), :], sem_out.at[h]) for h in range(2)]
            stores[0].start()
        ids_in[1].wait()
        @pl.when(fits)
        def _():
            bisect(1, lambda g, q: [(2 * m, lambda m=m: scatter(0, g, q * (SUB // 2) + m, 1, m)) for m in range(SUB // 2)])

        @pl.when(jnp.logical_not(fits))
        def _():
            bisect(1, lambda g, q: [])

        loop(0, part, lambda g: allocate(1, g))
        if second:
            stores[1].start()

        @pl.when(fits)
        def _():
            loop(0, part, lambda g: scatter(1, g, 0, SUB))

        @pl.when(jnp.logical_not(fits))
        def _():
            def one(h, k):
                g = k // group_rows
                j = k - g * group_rows
                s = j // blocks
                i = gidx[j * groups + h * part + g]
                r = g * group_rows + (j - s * blocks) * SUB + s
                acc_even[pl.ds(i, 1), :] = acc_even[pl.ds(i, 1), :] + works[h][pl.ds(r, 1), :]

            for h in range(2):
                loop(0, part_rows, lambda k: one(h, k))

        def finish(i, c):
            r = pl.multiple_of(i * SUB, SUB)
            for out, o in ((keep, 0), (send, half)):
                out[pl.ds(r, SUB), :] = (
                    (acc_even[pl.ds(r + o, SUB), :] + acc_odd[pl.ds(r + o, SUB), :])
                    + (acc_even[pl.ds(r + (full + o), SUB), :] + acc_odd[pl.ds(r + (full + o), SUB), :]))
            return c

        lax.fori_loop(0, half // SUB, finish, 0, unroll=8)

        def finish_copy(t, c):
            def more(i, c):
                r = pl.multiple_of(i * SUB, SUB)
                a = pl.multiple_of(t * full + r, SUB)
                for out, o in ((keep, 0), (send, half)):
                    out[pl.ds(r, SUB), :] += acc_even[pl.ds(a + o, SUB), :] + acc_odd[pl.ds(a + o, SUB), :]
                return c

            return lax.fori_loop(0, half // SUB, more, c, unroll=8)

        lax.fori_loop(2, used, finish_copy, 0)
        if second:
            for store in stores:
                store.wait()

    smem = pl.BlockSpec(memory_space=pltpu.SMEM)
    vmem = pl.BlockSpec(memory_space=pltpu.VMEM)
    left = pl.BlockSpec(memory_space=pltpu.HBM)
    outs = [jax.ShapeDtypeStruct((half, BLOCK), f32)] * 2
    out_specs = [vmem] * 2
    scratch = [
        pltpu.VMEM((full, BLOCK), f32),
        pltpu.VMEM((part_rows, BLOCK), f32),
        pltpu.VMEM((part_rows, BLOCK), f32),
        pltpu.VMEM((COPIES * full, BLOCK), f32),
        pltpu.VMEM((COPIES * full, BLOCK), f32),
        pltpu.VMEM((members, BLOCK), f32),
        pltpu.VMEM((members, BLOCK), f32),
        pltpu.VMEM((members, BLOCK), f32),
        pltpu.VMEM((part * SUB, BLOCK), f32),
        pltpu.VMEM((rows_all, BLOCK), f32),
        pltpu.VMEM((rows_all, BLOCK), f32),
        pltpu.SMEM((rows_all,), jnp.int32),
        pltpu.SMEM((rows_all,), jnp.int32),
        pltpu.SemaphoreType.DMA((pieces + 1, 2)),
        pltpu.SemaphoreType.DMA((2,)),
    ]
    if second:
        outs += [jax.ShapeDtypeStruct((rows_all, BLOCK), f32), jax.ShapeDtypeStruct((SUB, BLOCK), f32)]
        out_specs += [left, vmem]
        scratch += [pltpu.VMEM((rows_all, BLOCK), f32), pltpu.SemaphoreType.DMA((2,))]
    tables = [vmem] * (4 if second else 2)
    call = pl.pallas_call(
        body,
        out_shape=outs,
        in_specs=[left, left, smem] + tables + [left, left, vmem],
        out_specs=out_specs,
        scratch_shapes=scratch,
        compiler_params=pltpu.CompilerParams(vmem_limit_bytes=48 << 20),
        name="iterate2" if second else "iterate1",
    )

    def run(gidx, sidx, ncopy, *rest):
        *tables, aff, exp, nlive = rest
        aff, exp = (pltpu.with_memory_space_constraint(x, pltpu.HBM) for x in (aff, exp))
        return call(gidx, sidx, ncopy, *tables, aff, exp, nlive)

    return run


def vmem_call(body, name, *outs):
    spec = pl.BlockSpec(memory_space=pltpu.VMEM)
    return pl.pallas_call(
        body,
        out_shape=[jax.ShapeDtypeStruct(shape, jnp.float32) for shape in outs],
        out_specs=[spec] * len(outs),
        compiler_params=pltpu.CompilerParams(vmem_limit_bytes=4 << 20),
        name=name,
    )


def spread_duals(x, chips, core):
    own_rows = x.shape[0]

    def body(x, core, every):
        for p in range(chips):
            every[pl.ds(p * own_rows, own_rows), :] = x[...]

    return vmem_call(body, "spread_duals", (chips * own_rows, BLOCK))(
        x, jnp.full((SUB, BLOCK), core, jnp.int32))[0]


def sum_chips(x, chips):
    own_rows = x.shape[0] // chips

    def body(x, out):
        parts = [x[pl.ds(p * own_rows, own_rows), :] for p in range(chips)]
        while len(parts) > 1:
            parts = [a + b for a, b in zip(parts[::2], parts[1::2])]
        out[...] = parts[0]

    return vmem_call(body, "sum_chips", (own_rows, BLOCK))(x)[0]


def gradient_of(plane, shifted, limit):
    one, two, three = shifted
    return ((plane[...] + two[...]) + (one[...] + three[...])) - limit[...]


def spread_gradient(plane, shifted, limit, chips):
    own_rows = plane.shape[0]

    def body(plane, one, two, three, limit, gradient, every):
        g = gradient_of(plane, (one, two, three), limit)
        gradient[...] = g
        for p in range(chips):
            every[pl.ds(p * own_rows, own_rows), :] = g

    return vmem_call(body, "spread_gradient", plane.shape, (chips * own_rows, BLOCK))(plane, *shifted, limit)


def last_gradient(plane, shifted, limit, shards):
    def body(plane, one, two, three, limit, gradient, parts):
        g = gradient_of(plane, (one, two, three), limit)
        gradient[...] = g
        part = jnp.sum(jnp.sum(g * g, axis=0, keepdims=True), axis=1, keepdims=True)
        parts[...] = jnp.broadcast_to(part[None], parts.shape)

    return vmem_call(body, "last_gradient", plane.shape, (shards, 1, BLOCK))(plane, *shifted, limit)


def last_duals(duals, first, sumsq, second, parts, item_count):
    def body(duals, first, sumsq, second, parts, out):
        scale = jnp.sqrt(sumsq[0:1, :] / item_count + 1e-6)
        lam = jnp.maximum(duals[...] + 0.5 * first[...] / scale, 0.0)
        scale = jnp.sqrt(jnp.sum(parts[...], axis=0) / item_count + 1e-6)
        out[...] = jnp.maximum(lam + 0.5 * second[...] / scale, 0.0)

    return vmem_call(body, "last_duals", duals.shape)(duals, first, sumsq, second, parts)[0]


def local(candidates, affinity, exposure, lengths, item_limit, item_duals, *, grp_size, shard_size):
    chips = shard_size // 2
    same_core = [[2 * p + c for p in range(chips)] for c in range(2)]
    swap = [(g * shard_size + s, g * shard_size + (s ^ 1)) for g in range(grp_size) for s in range(shard_size)]
    members, slots = affinity.shape
    blocks = slots // BLOCK
    groups = members // SUB
    own_items = item_limit.shape[0]
    item_count = own_items * shard_size
    own_rows = own_items // BLOCK
    half = chips * own_rows
    full = 2 * half
    core = lax.axis_index("shard") % 2

    def swap_cores(x):
        return lax.ppermute(x, AXES, swap)

    def as_rows(x):
        return x.reshape(groups, SUB, blocks, BLOCK).transpose(0, 2, 1, 3).reshape(-1, BLOCK)

    def exchange(x):
        x = x.reshape(chips, 1, own_items)
        return lax.all_to_all(
            x, "shard", 0, 0, axis_index_groups=same_core, tiled=True).reshape(half, BLOCK)

    def gather_halves(every):
        every = exchange(every)
        return every, swap_cores(every)

    def reduce_loads(keep, send):
        chip = keep + swap_cores(send)
        plane = sum_chips(exchange(chip), chips)
        return plane, [
            lax.ppermute(plane, "grp", [(g, (g + d) % grp_size) for g in range(grp_size)])
            for d in range(1, grp_size)
        ]

    shard_of = candidates // own_rows
    gidx = (jnp.where(shard_of % 2 == core, 0, half) + (shard_of // 2) * own_rows + candidates % own_rows).reshape(-1)
    batch = gidx.reshape(-1, blocks)
    earlier = jnp.arange(blocks)[:, None] > jnp.arange(blocks)[None, :]
    copy = jnp.sum((batch[:, :, None] == batch[:, None, :]) & earlier, axis=2, dtype=jnp.int32)
    sidx = (batch + full * copy).reshape(groups, -1).T.reshape(-1)
    gidx = gidx.reshape(groups, -1).T.reshape(-1)
    ncopy = (jnp.max(copy) + 1).reshape(1)

    aff = as_rows(affinity)
    exp = as_rows(exposure)
    nlive = jnp.broadcast_to((lengths // BLOCK)[:, None], (members, BLOCK))
    limit = item_limit.reshape(own_rows, BLOCK)
    duals = item_duals.reshape(own_rows, BLOCK)

    own_d, other_d = gather_halves(spread_duals(duals, chips, core))
    keep, send = iteration_kernel(False, groups, blocks, half, item_count)(
        gidx, sidx, ncopy, own_d, other_d, aff, exp, nlive)
    first, every = spread_gradient(*reduce_loads(keep, send), limit, chips)

    own_g, other_g = gather_halves(every)
    keep, send, primal, sumsq = iteration_kernel(True, groups, blocks, half, item_count)(
        gidx, sidx, ncopy, own_d, other_d, own_g, other_g, aff, exp, nlive)
    second, parts = last_gradient(*reduce_loads(keep, send), limit, shard_size)
    parts = lax.all_to_all(parts, "shard", 0, 0, tiled=True)
    duals = last_duals(duals, first, sumsq, second, parts, item_count)

    primal = primal.reshape(groups, blocks, SUB, BLOCK).transpose(0, 2, 1, 3).reshape(members, slots)
    return primal, duals.reshape(-1)


def solution(mesh):
    placed = (
        P(("grp", "shard"), None),
        P(("grp", "shard"), None),
        P(("grp", "shard"), None),
        P(("grp", "shard")),
        P("shard"),
        P("shard"),
    )

    def run(*args):
        return local(*args, grp_size=mesh.shape["grp"], shard_size=mesh.shape["shard"])

    return jax.shard_map(
        run,
        mesh=mesh,
        in_specs=placed,
        out_specs=(P(("grp", "shard"), None), P("shard")),
        check_vma=False,
    )
```
